128 devices in a mesh: chan: 8 (over x, core), vox: 16 (over z, y).
Axes of the slice: x: 4, y: 4, z: 4, core: 2. Of those that a mesh axis runs over, the one named last changes fastest.
Arguments:
- features: bfloat16 [512, 5632], P('chan'), may hold values from -6 to 6
- hrf_filters: float32 [3, 5632, 16], P(None, 'chan'), may hold values from -1.5 to 1.5
- weights: bfloat16 [3, 5632, 81920], P(None, 'chan', 'vox'), may hold values from -0.046875 to 0.046875
- voxel_parcel: int32 [81920], P('vox'), may hold values from 0 to 1599, as said below
- parcel_owner: int32 [1600], replicated, may hold values from 0 to 15, as said below
Outputs:
- owned: bfloat16 [256, 640, 512], P('vox', None, 'chan')
The draws below stay inside these ranges and needn't reach their ends.
Inputs may be any that keep to these rules, and one draw needn't show every extreme that they name: `voxel_parcel`: among the 5120 voxels of one index of vox, at most 640 belong to parcels of one owner, and some owner gets exactly 640; one owner gets exactly 640 from every index of vox. `parcel_owner`: every owner holds exactly 100 parcels.
All inputs are finite; a program needn't handle non-finite values.
Results may differ from the reference program's by a relative error of at most 0.01.
Values may be sent and summed in bfloat16 or wider, within the bound.
A program may use at most 128 MiB of HBM per device.

```python
import jax
import jax.numpy as jnp
from jax import lax

CH = 5632
BASES = 3
FILTER_TAPS = 16
TAP_SPACING = 2
TIME = 512
VOX_DEV = 5120
VOXELS = 81920
SEND = 640
PAR_OWNER = 100
PARCELS = 1600
N_CHAN = 8
N_VOX = 16


def one_permutation(derived_key, count):
    return jax.random.permutation(derived_key, count)


def parcel_tables(key):
    base = jax.random.fold_in(key, 11)
    key_perm, key_rank, key_star, key_shuffle, key_first, key_second = jax.random.split(base, 6)
    shuffled_ids = jax.random.permutation(key_perm, PARCELS).astype(jnp.int32)
    parcel_owner = (shuffled_ids % N_VOX).astype(jnp.int32)
    inverse = jnp.argsort(shuffled_ids).astype(jnp.int32)
    ranked = jax.vmap(lambda derived_key: one_permutation(derived_key, N_VOX))(jax.random.split(key_rank, N_VOX)).astype(jnp.int32)
    central_holder = jax.random.randint(key_star, (), 0, N_VOX).astype(jnp.int32)
    ranked = (ranked + central_holder - ranked[:, :1]) % N_VOX
    position = jnp.arange(VOX_DEV, dtype=jnp.int32)
    quarter = N_VOX // 4
    edge_one = quarter * SEND
    edge_two = edge_one + quarter * (SEND // 2)
    rank_of = jnp.where(position < edge_one, position // SEND, jnp.where(position < edge_two, quarter + (position - edge_one) // (SEND // 2), 2 * quarter + (position - edge_two) // (SEND // 4)))
    owner_seq = ranked[:, rank_of]
    shuffle = jax.vmap(lambda derived_key: one_permutation(derived_key, VOX_DEV))(jax.random.split(key_shuffle, N_VOX)).astype(jnp.int32)
    voxel_owner = jnp.take_along_axis(owner_seq, shuffle, axis=1)
    first_draw = jax.random.randint(key_first, (N_VOX, VOX_DEV), 0, PAR_OWNER).astype(jnp.int32)
    second_draw = jax.random.randint(key_second, (N_VOX, VOX_DEV), 0, PAR_OWNER).astype(jnp.int32)
    member = first_draw * second_draw // PAR_OWNER
    voxel_parcel = inverse[member * N_VOX + voxel_owner].reshape(-1)
    return (voxel_parcel.astype(jnp.int32), parcel_owner)


def draw_voxel_parcel(key, part):
    return parcel_tables(key)[0]


def draw_parcel_owner(key, part):
    return parcel_tables(key)[1]


def shard_levels(rng, extent, shards, low, largest):
    loudness = 1.0
    for dim, blocks in shards:
        draws = jax.random.uniform(jax.random.fold_in(jax.random.fold_in(rng, 6), dim), (blocks,), jnp.float32, low / len(shards), largest / len(shards))
        loudness = loudness * jnp.repeat(jnp.exp(draws), extent[dim] // blocks).reshape((-1,) + (1,) * (len(extent) - 1 - dim))
    return loudness


def noise(key, dims, width, bound, cuts=(), kind=jnp.bfloat16):
    factor_of = shard_levels(key, dims, cuts, -0.22, 0.18) if cuts else 1.0
    array = jax.random.normal(key, dims, jnp.float32) * width * factor_of
    return jnp.minimum(jnp.maximum(array, -bound), bound).astype(kind)


def setup_inputs(seed: int = 0) -> dict:
    key_list = jax.random.split(jax.random.key(seed), 6)
    features = noise(key_list[0], (TIME, CH), 1.0, 6.0, ((0, 8),))
    hrf_filters = noise(key_list[1], (BASES, CH, FILTER_TAPS), FILTER_TAPS ** -0.5, 1.5, ((1, 8),), jnp.float32)
    weights = noise(key_list[2], (BASES, CH, VOXELS), (BASES * CH) ** -0.5, 0.046875, ((1, 8), (2, 16)))
    voxel_parcel = draw_voxel_parcel(jax.random.fold_in(key_list[5], 71), 0)
    parcel_owner = draw_parcel_owner(jax.random.fold_in(key_list[5], 71), 0)
    return dict(features=features, hrf_filters=hrf_filters, weights=weights, voxel_parcel=voxel_parcel, parcel_owner=parcel_owner)


def reference(features, hrf_filters, weights, voxel_parcel, parcel_owner):
    series = features.astype(jnp.float32).T
    largest_delay = TAP_SPACING * (FILTER_TAPS - 1)
    padded = jnp.pad(series, ((0, 0), (largest_delay, 0)))
    filtered = jnp.zeros((BASES, CH, TIME), jnp.float32)
    for delay_index in range(FILTER_TAPS):
        window_start = largest_delay - TAP_SPACING * delay_index
        lagged = padded[:, window_start:window_start + TIME]
        filtered = filtered + hrf_filters[:, :, delay_index][:, :, None] * lagged[None]
    design = filtered.astype(jnp.bfloat16)
    chan_width = CH // N_CHAN

    def add_block(running, block_index):
        start = (block_index * chan_width).astype(jnp.int32)
        design_block = lax.dynamic_slice_in_dim(design, start, chan_width, 1).reshape(BASES * chan_width, TIME)
        weight_block = lax.dynamic_slice_in_dim(weights, start, chan_width, 1).reshape(BASES * chan_width, VOXELS)
        partial_value = lax.dot_general(weight_block, design_block, (((0,), (0,)), ((), ())), preferred_element_type=jnp.float32)
        rounded = lax.optimization_barrier(partial_value.astype(jnp.bfloat16))
        return running + rounded.astype(jnp.float32), None

    running, _ = lax.scan(add_block, jnp.zeros((VOXELS, TIME), jnp.float32), jnp.arange(N_CHAN, dtype=jnp.int32))
    predicted = running.astype(jnp.bfloat16)
    parcel_holders = parcel_owner[voxel_parcel].astype(jnp.int32)
    grouped = parcel_holders.reshape(N_VOX, VOX_DEV)
    onehot = (grouped[:, :, None] == jnp.arange(N_VOX, dtype=jnp.int32)[None, None, :]).astype(jnp.int32)
    before = jnp.cumsum(onehot, axis=1) - onehot
    slot_index = jnp.sum(before * onehot, axis=2)
    source = jnp.arange(N_VOX, dtype=jnp.int32)[:, None]
    target_row = ((grouped * N_VOX + source) * SEND + slot_index).reshape(-1).astype(jnp.int32)
    owned = jnp.zeros((N_VOX * N_VOX * SEND, TIME), jnp.bfloat16).at[target_row].set(predicted)
    return owned.reshape(N_VOX * N_VOX, SEND, TIME)
```

```python
import functools

import jax
import jax.numpy as jnp
from jax import lax
from jax.experimental import pallas as pl
from jax.experimental.pallas import tpu as pltpu
from jax.sharding import PartitionSpec as P

MESH = pl.DeviceIdType.MESH
TAP_SPACING = 2
VMEM_LIMIT = 66_000_000
LANES = 128
SLAB = 512
SORT = 256
TILE = 8
LOCAL_TILES = 60
GROUP = 12
LAG = 2


def up(value, multiple):
    return -(-value // multiple) * multiple


def main_kernel(
    sizes,
    feat_ref, hrf_ref, w_ref, out_ref,
    wv, fe, series, coef, design, own, dsend, drecv, rsend, rrecv,
    w_sem, f_local, f_send, f_recv, d_send, d_recv, r_send, r_recv,
):
    n_chan, bases, taps, width, wide, block, steps = sizes
    pairs = n_chan // 2
    half = SLAB // 2
    me = lax.axis_index("chan")
    chip = me // 2
    core = me % 2
    partner = chip * 2 + (1 - core)
    right = lax.rem(chip + 1, pairs) * 2 + core
    left = lax.rem(chip + pairs - 1, pairs) * 2 + core
    shift = core * (wide - width)

    def weight_copy(i):
        cols = pl.ds(pl.multiple_of(i * SLAB, SLAB), SLAB)
        rows = pl.ds(pl.multiple_of(shift, 64), width)
        return pltpu.make_async_copy(w_ref.at[:, :, cols], wv.at[:, rows, cols], w_sem.at[i])

    def window(k):
        start = k * width - lax.rem(k, 2) * (wide - width)
        return pl.ds(pl.multiple_of(start, LANES), wide)

    local = pltpu.make_async_copy(feat_ref.at[:, window(me)], fe.at[me], f_local)
    local.start()

    barrier = pltpu.get_barrier_semaphore()
    for d in range(1, n_chan):
        pl.semaphore_signal(
            barrier, inc=1, device_id={"chan": lax.rem(me + d, n_chan)}, device_id_type=MESH
        )
    pl.semaphore_wait(barrier, n_chan - 1)

    def feature_copy(d):
        peer = lax.rem(me + d, n_chan)
        return pltpu.make_async_remote_copy(
            src_ref=feat_ref.at[:, window(peer)],
            dst_ref=fe.at[me],
            send_sem=f_send.at[d - 1],
            recv_sem=f_recv.at[d - 1],
            device_id={"chan": peer},
            device_id_type=MESH,
        )

    for d in (4, 3, 5, 2, 6, 1, 7):
        if d < n_chan:
            feature_copy(d).start()

    @pl.loop(0, steps)
    def _(i):
        weight_copy(i).start()

    blank = pl.ds(pl.multiple_of((1 - core) * width, 64), wide - width)
    for b in range(bases):
        wv[b, blank, :] = jnp.zeros((wide - width, wv.shape[2]), wv.dtype)
    coef[...] = jnp.zeros(coef.shape, coef.dtype)

    @pl.when(core == 0)
    def _():
        coef[:, :, :width] = hrf_ref[...]

    @pl.when(core == 1)
    def _():
        coef[:, :, wide - width :] = hrf_ref[...]

    pad = 32
    series[:pad, :] = jnp.zeros((pad, wide), jnp.float32)
    local.wait()
    for d in range(1, n_chan):
        feature_copy(d).wait_recv()

    @pl.loop(0, n_chan)
    def _(r):
        rows = pl.ds(pl.multiple_of(pad + r * block, 32), block)
        series[rows, :] = fe[r].astype(jnp.float32)

    span = 32

    @pl.loop(0, n_chan * block // span)
    def _(s):
        r = s // (block // span)
        sub = lax.rem(s, block // span)
        other = (lax.rem(r, 2) - core) * (lax.rem(r, 2) - core)
        row = (other * pairs + r // 2) * block + sub * span
        rows = pl.ds(pl.multiple_of(row, span), span)
        for lane in range(wide // LANES):
            lanes = slice(lane * LANES, (lane + 1) * LANES)
            past = series[pl.ds(pl.multiple_of(s * span, span), pad + span), lanes]
            lagged = [past] + [pltpu.roll(past, TAP_SPACING * m, 0) for m in range(1, 4)]
            for b in range(bases):
                total = None
                for j in range(taps):
                    start = pad - TILE * (j // 4)
                    term = coef[b, j : j + 1, lanes] * lagged[j % 4][start : start + span]
                    total = term if total is None else total + term
                cols = slice(b * wide + lane * LANES, b * wide + (lane + 1) * LANES)
                design[rows, cols] = total.astype(design.dtype)

    def pair_copy(i):
        cols = pl.ds(pl.multiple_of(i * SLAB, SLAB), SLAB)
        return pltpu.make_async_remote_copy(
            src_ref=dsend.at[:, cols], dst_ref=drecv.at[:, cols],
            send_sem=d_send.at[i], recv_sem=d_recv.at[i],
            device_id={"chan": partner}, device_id_type=MESH,
        )

    def ring_copy(step, way, i):
        cols = pl.ds(pl.multiple_of(i * SLAB + way * half, half), half)
        return pltpu.make_async_remote_copy(
            src_ref=rsend.at[step, :, cols], dst_ref=rrecv.at[step, :, cols],
            send_sem=r_send.at[step, way, i], recv_sem=r_recv.at[step, way, i],
            device_id={"chan": (right, left)[way]}, device_id_type=MESH,
        )

    def own_part(step, way, i):
        away = pairs - 1 - step if way == 0 else step + 1
        target = lax.rem(chip + away, pairs)
        rows = pl.ds(pl.multiple_of(target * block, block), block)
        cols = pl.ds(pl.multiple_of(i * SLAB + way * half, half), half)
        return own[rows, cols]

    def ring_cols(way, i):
        return pl.ds(pl.multiple_of(i * SLAB + way * half, half), half)

    mine = pairs * block

    def multiply(i):
        weight_copy(i).wait()
        for h in range(SLAB // 256):
            cols = pl.ds(pl.multiple_of(i * SLAB + h * 256, 256), 256)
            panel = wv[:, :, cols].reshape(bases * wide, 256)
            product = jnp.dot(design[...], panel, preferred_element_type=jnp.float32)
            dsend[:, cols] = product[mine:].astype(dsend.dtype)
            own[:, cols] = product[:mine]
        pair_copy(i).start()

    def pair_sum(i):
        pair_copy(i).wait_recv()
        cols = pl.ds(pl.multiple_of(i * SLAB, SLAB), SLAB)
        own[:, cols] = own[:, cols] + drecv[:, cols].astype(jnp.float32)
        for way in range(2):
            rsend[0, :, ring_cols(way, i)] = own_part(0, way, i).astype(rsend.dtype)
            ring_copy(0, way, i).start()

    def pass_on(step, i):
        for way in range(2):
            ring_copy(step - 1, way, i).wait_recv()
            cols = ring_cols(way, i)
            total = own_part(step, way, i) + rrecv[step - 1, :, cols].astype(jnp.float32)
            if step < pairs - 1:
                rsend[step, :, cols] = total.astype(rsend.dtype)
                ring_copy(step, way, i).start()
            else:
                out_ref[:, cols] = total.astype(out_ref.dtype)

    last = 1 + (pairs - 1) * LAG

    @pl.loop(0, steps + last)
    def _(it):
        @pl.when(it < steps)
        def _():
            multiply(it)

        @pl.when(jnp.logical_and(it >= 1, it < steps + 1))
        def _():
            pair_sum(it - 1)

        for step in range(1, pairs):
            lag = 1 + step * LAG

            @pl.when(jnp.logical_and(it >= lag, it < steps + lag))
            def _(step=step, lag=lag):
                pass_on(step, it - lag)

    for d in range(1, n_chan):
        feature_copy(d).wait_send()

    @pl.loop(0, steps)
    def _(i):
        pair_copy(i).wait_send()
        for step in range(pairs - 1):
            for way in range(2):
                ring_copy(step, way, i).wait_send()


def predicted_block(features, hrf_filters, weights, n_chan):
    block, _ = features.shape
    bases, width, taps = hrf_filters.shape
    voxels = weights.shape[2]
    wide = up(width, LANES)
    steps = voxels // SLAB
    pairs = n_chan // 2
    sizes = (n_chan, bases, taps, width, wide, block, steps)
    hbm = pl.BlockSpec(memory_space=pl.ANY)
    vmem = pl.BlockSpec(memory_space=pltpu.VMEM)
    dma = pltpu.SemaphoreType.DMA
    return pl.pallas_call(
        functools.partial(main_kernel, sizes),
        out_shape=jax.ShapeDtypeStruct((block, voxels), jnp.bfloat16),
        in_specs=[hbm, vmem, hbm],
        out_specs=vmem,
        scratch_shapes=[
            pltpu.VMEM((bases, wide, voxels), jnp.bfloat16),
            pltpu.VMEM((n_chan, block, wide), jnp.bfloat16),
            pltpu.VMEM((32 + n_chan * block, wide), jnp.float32),
            pltpu.VMEM((bases, taps, wide), jnp.float32),
            pltpu.VMEM((n_chan * block, bases * wide), jnp.bfloat16),
            pltpu.VMEM((pairs * block, voxels), jnp.float32),
            pltpu.VMEM((pairs * block, voxels), jnp.bfloat16),
            pltpu.VMEM((pairs * block, voxels), jnp.bfloat16),
            pltpu.VMEM((pairs - 1, block, voxels), jnp.bfloat16),
            pltpu.VMEM((pairs - 1, block, voxels), jnp.bfloat16),
            dma((steps,)),
            dma,
            dma((n_chan - 1,)),
            dma((n_chan - 1,)),
            dma((steps,)),
            dma((steps,)),
            dma((pairs - 1, 2, steps)),
            dma((pairs - 1, 2, steps)),
        ],
        compiler_params=pltpu.CompilerParams(
            collective_id=0, has_side_effects=True, vmem_limit_bytes=VMEM_LIMIT
        ),
        name="predict",
    )(features, hrf_filters.transpose(0, 2, 1), weights)


def route_kernel(owners, cap, vp_ref, table_ref, place_ref, dest_ref):
    groups = vp_ref.shape[0]
    parcel = vp_ref[...]
    high = parcel // LANES
    low = parcel - high * LANES
    owner_parts = []
    for h in range(SORT // LANES):
        lanes = slice(h * LANES, (h + 1) * LANES)
        found = jnp.full((groups, LANES), -1, jnp.int32)
        index = low[:, lanes]
        for row in range(table_ref.shape[0]):
            entries = jnp.broadcast_to(table_ref[row : row + 1, :], (groups, LANES))
            value = jnp.take_along_axis(entries, index, axis=1)
            found = jnp.where(high[:, lanes] == row, value, found)
        owner_parts.append(found)
    owner = jnp.concatenate(owner_parts, axis=1)

    def before(n):
        return (
            lax.broadcasted_iota(jnp.int32, (n, n), 0) < lax.broadcasted_iota(jnp.int32, (n, n), 1)
        )

    def ones(mask):
        return jnp.where(mask, 1.0, 0.0).astype(jnp.bfloat16)

    ahead = ones(before(SORT))
    lane = lax.broadcasted_iota(jnp.int32, (groups, LANES), 1)
    counts = jnp.zeros((groups, LANES), jnp.float32)
    ranks = []
    for o in range(owners):
        mask = jnp.where(owner == o, 1.0, 0.0)
        ranks.append(
            jnp.dot(mask.astype(jnp.bfloat16), ahead, preferred_element_type=jnp.float32)
        )
        counts = jnp.where(lane == o, jnp.sum(mask, axis=1, keepdims=True), counts)
    earlier = ones(
        lax.broadcasted_iota(jnp.int32, (groups, groups), 0)
        > lax.broadcasted_iota(jnp.int32, (groups, groups), 1)
    )
    start = jnp.dot(earlier, counts.astype(jnp.bfloat16), preferred_element_type=jnp.float32)
    start = start.astype(jnp.int32)
    counts = counts.astype(jnp.int32)
    first = start >> 3
    phase = start & 7
    tiles = jnp.where(counts > 0, (phase + counts + 7) >> 3, 0)
    tile_start = jnp.dot(
        tiles.astype(jnp.float32).astype(jnp.bfloat16), ones(before(LANES)),
        preferred_element_type=jnp.float32,
    ).astype(jnp.int32)

    def column(values, o):
        return jnp.sum(jnp.where(lane == o, values, 0), axis=1, keepdims=True)

    place = jnp.full((groups, SORT), -1, jnp.int32)
    dest = jnp.full((groups, LANES), owners * cap // TILE, jnp.int32)
    for o in range(owners):
        offset = column(tile_start * TILE + phase, o)
        place = jnp.where(owner == o, offset + ranks[o].astype(jnp.int32), place)
        low_tile = column(tile_start, o)
        top_tile = low_tile + column(tiles, o)
        spot = o * (cap // TILE) + column(first, o) + lane - low_tile
        dest = jnp.where(jnp.logical_and(lane >= low_tile, lane < top_tile), spot, dest)
    place_ref[...] = place
    dest_ref[...] = dest


def routes(voxel_parcel, parcel_owner, owners, cap):
    voxels = voxel_parcel.shape[0]
    groups = voxels // SORT
    rows = up(groups, 8)
    parcels = jnp.pad(
        voxel_parcel.reshape(groups, SORT), ((0, rows - groups), (0, 0)), constant_values=-1
    )
    entries = up(parcel_owner.shape[0], LANES)
    table = jnp.pad(parcel_owner, (0, entries - parcel_owner.shape[0])).reshape(-1, LANES)
    return pl.pallas_call(
        functools.partial(route_kernel, owners, cap),
        out_shape=(
            jax.ShapeDtypeStruct((rows, SORT), jnp.int32),
            jax.ShapeDtypeStruct((rows, LANES), jnp.int32),
        ),
        name="route",
    )(parcels, table)


def pack_kernel(groups, owners, dest_ref, place_ref, pred_ref, out_ref, buf, loc):
    block = pred_ref.shape[0]
    zero = jnp.zeros((64, LANES), jnp.float32)

    @pl.loop(0, buf.shape[0] // 64)
    def _(i):
        buf[pl.ds(pl.multiple_of(i * 64, 64), 64), :] = zero

    local_rows = LOCAL_TILES * TILE

    @pl.loop(0, groups)
    def _(g):
        place = place_ref[pl.ds(g, 1), :]
        row = lax.broadcasted_iota(jnp.int32, (local_rows, SORT), 0)
        select = jnp.where(row == place, 1.0, 0.0).astype(jnp.bfloat16)
        part = pred_ref[:, pl.ds(pl.multiple_of(g * SORT, SORT), SORT)]
        twice = jnp.concatenate([part, part], axis=0)
        loc[...] = lax.dot_general(
            select, twice, (((1,), (1,)), ((), ())), preferred_element_type=jnp.float32
        )
        for base in range(0, LOCAL_TILES, GROUP):
            places = [
                pl.ds(pl.multiple_of(dest_ref[g, base + k] * TILE, TILE), TILE)
                for k in range(GROUP)
            ]
            held = [
                buf[spot, :] + loc[(base + k) * TILE : (base + k + 1) * TILE, :]
                for k, spot in enumerate(places)
            ]
            for spot, value in zip(places, held):
                buf[spot, :] = value

    left = lax.broadcasted_iota(jnp.int32, (LANES, LANES), 1) < block
    pairs = owners // 2
    cap = out_ref.shape[2]

    @pl.loop(0, pairs)
    def _(p):
        for tile in range(cap // LANES):
            here = pl.multiple_of(p * cap + tile * LANES, LANES)
            first = buf[pl.ds(here, LANES), :]
            second = buf[pl.ds(pl.multiple_of(pairs * cap + here, LANES), LANES), :]
            both = jnp.where(left, first, second).T.astype(out_ref.dtype)
            cols = slice(tile * LANES, (tile + 1) * LANES)
            out_ref[p, :, cols] = both[:block]
            out_ref[pairs + p, :, cols] = both[block:]


def packed_slots(predicted, place, dest, owners, cap):
    block, voxels = predicted.shape
    vmem = pl.BlockSpec(memory_space=pltpu.VMEM)
    return pl.pallas_call(
        functools.partial(pack_kernel, voxels // SORT, owners),
        out_shape=jax.ShapeDtypeStruct((owners, block, cap), jnp.bfloat16),
        in_specs=[pl.BlockSpec(memory_space=pltpu.SMEM), vmem, vmem],
        out_specs=vmem,
        scratch_shapes=[
            pltpu.VMEM((owners * cap + 64, LANES), jnp.float32),
            pltpu.VMEM((LOCAL_TILES * TILE, LANES), jnp.float32),
        ],
        compiler_params=pltpu.CompilerParams(vmem_limit_bytes=32_000_000),
        name="pack",
    )(dest, place, predicted)


def shards(features, hrf_filters, weights, voxel_parcel, parcel_owner):
    owners = lax.axis_size("vox")
    cap = 2 * voxel_parcel.shape[0] // owners
    place, dest = routes(voxel_parcel, parcel_owner, owners, cap)
    predicted = predicted_block(features, hrf_filters, weights, lax.axis_size("chan"))
    packed = packed_slots(predicted, place, dest, owners, cap)
    received = lax.all_to_all(packed, "vox", split_axis=0, concat_axis=0, tiled=True)
    return received.transpose(0, 2, 1)


def solution(mesh):
    return jax.shard_map(
        shards,
        mesh=mesh,
        in_specs=(P("chan", None), P(None, "chan", None), P(None, "chan", "vox"), P("vox"), P()),
        out_specs=P("vox", None, "chan"),
        check_vma=False,
    )
```

```python
import functools

import jax
import jax.numpy as jnp
from jax import lax
from jax.experimental import pallas as pl
from jax.experimental.pallas import tpu as pltpu
from jax.sharding import PartitionSpec as P

MESH = pl.DeviceIdType.MESH
TAP_SPACING = 2
VMEM_LIMIT = 66_000_000
LANES = 128
SLAB = 512
SORT = 256
TILE = 8
LOCAL_TILES = 60
GROUP = 12
LAGS = (1, 3, 6, 10)


def up(value, multiple):
    return -(-value // multiple) * multiple


def main_kernel(
    sizes,
    feat_ref, hrf_ref, w_ref, out_ref,
    wv, fe, series, hrf, coef, design, own, dsend, drecv, rsend, rrecv, done,
    w_sem, h_sem, f_local, f_send, f_recv, d_send, d_recv, r_send, r_recv, o_sem,
):
    n_chan, bases, taps, width, wide, block, steps = sizes
    pairs = n_chan // 2
    half = SLAB // 2
    me = lax.axis_index("chan")
    chip = me // 2
    core = lax.rem(me, 2)

    def device(away, flip):
        return lax.rem(chip + away, pairs) * 2 + (core if flip == 0 else 1 - core)

    shift = core * (wide - width)

    def weight_copy(i):
        cols = pl.ds(pl.multiple_of(i * SLAB, SLAB), SLAB)
        rows = pl.ds(pl.multiple_of(shift, 64), width)
        return pltpu.make_async_copy(w_ref.at[:, :, cols], wv.at[:, rows, cols], w_sem.at[i])

    def window(k):
        start = k * width - lax.rem(k, 2) * (wide - width)
        return pl.ds(pl.multiple_of(start, LANES), wide)

    local = pltpu.make_async_copy(feat_ref.at[:, window(me)], fe.at[me], f_local)
    local.start()
    taps_copy = pltpu.make_async_copy(hrf_ref, hrf, h_sem)
    taps_copy.start()

    barrier = pltpu.get_barrier_semaphore()
    for d in range(1, n_chan):
        pl.semaphore_signal(
            barrier, inc=1, device_id={"chan": lax.rem(me + d, n_chan)}, device_id_type=MESH
        )
    pl.semaphore_wait(barrier, n_chan - 1)

    parts = [(0, 1, 0, block)]
    parts += [(away, flip, 0, block) for away in (1, 3) for flip in (0, 1)]
    parts += [(2, flip, row, 32) for row in (32, 0) for flip in (0, 1)]

    def feature_copy(n):
        away, flip, row, rows = parts[n]
        peer = device(away, flip)
        return pltpu.make_async_remote_copy(
            src_ref=feat_ref.at[pl.ds(row, rows), window(peer)],
            dst_ref=fe.at[me, pl.ds(row, rows)],
            send_sem=f_send.at[n],
            recv_sem=f_recv.at[n],
            device_id={"chan": peer},
            device_id_type=MESH,
        )

    for n in range(len(parts)):
        feature_copy(n).start()

    @pl.loop(0, steps)
    def _(i):
        weight_copy(i).start()

    blank = pl.ds(pl.multiple_of((1 - core) * width, 64), wide - width)
    for b in range(bases):
        wv[b, blank, :] = jnp.zeros((wide - width, wv.shape[2]), wv.dtype)
    pad = 32
    series[:pad, :] = jnp.zeros((pad, wide), jnp.float32)

    def widen(source, row, rows):
        there = pl.ds(pl.multiple_of(pad + source * block + row, 32), rows)
        series[there, :] = fe[source, row : row + rows, :].astype(jnp.float32)

    def arrive(n):
        away, flip, row, rows = parts[n]
        feature_copy(n).wait_recv()
        widen(device(pairs - away, flip), row, rows)

    taps_copy.wait()
    coef[...] = jnp.zeros(coef.shape, coef.dtype)

    @pl.when(core == 0)
    def _():
        coef[:, :, :width] = hrf[...]

    @pl.when(core == 1)
    def _():
        coef[:, :, wide - width :] = hrf[...]

    local.wait()
    widen(me, 0, block)
    arrive(0)

    span = 32
    spans = block // span

    @pl.loop(0, n_chan * spans)
    def _(s):
        for when, some in ((spans, (1, 2, 3, 4)), (5 * spans, (5, 6)), (6 * spans, (7, 8))):

            @pl.when(s == when)
            def _(some=some):
                for n in some:
                    arrive(n)

        q = s // spans
        g = q // 3
        away = (1 + q) * (1 - g) * (2 - g) // 2 + (3 - q) * g * (2 - g) + (q - 2) * g * (g - 1) // 2
        r = lax.rem(chip * 2 + away + n_chan, n_chan)
        sub = lax.rem(s, spans)
        parity = lax.rem(r, 2)
        other = parity + core - 2 * parity * core
        row = (other * pairs + r // 2) * block + sub * span
        rows = pl.ds(pl.multiple_of(row, span), span)
        time = pl.multiple_of(r * block + sub * span, span)
        for lane in range(wide // LANES):
            lanes = slice(lane * LANES, (lane + 1) * LANES)
            past = series[pl.ds(time, pad + span), lanes]
            lagged = [past] + [pltpu.roll(past, TAP_SPACING * m, 0) for m in range(1, 4)]
            for b in range(bases):
                total = None
                for j in range(taps):
                    start = pad - TILE * (j // 4)
                    term = coef[b, j : j + 1, lanes] * lagged[j % 4][start : start + span]
                    total = term if total is None else total + term
                cols = slice(b * wide + lane * LANES, b * wide + (lane + 1) * LANES)
                design[rows, cols] = total.astype(design.dtype)

    mine = pairs * block

    def slab(i):
        return pl.ds(pl.multiple_of(i * SLAB, SLAB), SLAB)

    def way_cols(way, i):
        return pl.ds(pl.multiple_of(i * SLAB + way * half, half), half)

    def pair_copy(i):
        return pltpu.make_async_remote_copy(
            src_ref=dsend.at[:, slab(i)], dst_ref=drecv.at[:, slab(i)],
            send_sem=d_send.at[i], recv_sem=d_recv.at[i],
            device_id={"chan": device(0, 1)}, device_id_type=MESH,
        )

    def ring_copy(step, way, i):
        cols = way_cols(way, i)
        return pltpu.make_async_remote_copy(
            src_ref=rsend.at[step, :, cols], dst_ref=rrecv.at[step, :, cols],
            send_sem=r_send.at[step, way, i], recv_sem=r_recv.at[step, way, i],
            device_id={"chan": device((1, pairs - 1)[way], 0)}, device_id_type=MESH,
        )

    def out_copy(i):
        return pltpu.make_async_copy(done.at[:, slab(i)], out_ref.at[:, slab(i)], o_sem.at[i])

    def own_part(step, way, i):
        away = pairs - 1 - step if way == 0 else step + 1
        target = lax.rem(chip + away, pairs)
        return own[pl.ds(pl.multiple_of(target * block, block), block), way_cols(way, i)]

    def multiply(i):
        weight_copy(i).wait()
        for h in range(SLAB // 256):
            cols = pl.ds(pl.multiple_of(i * SLAB + h * 256, 256), 256)
            panel = wv[:, :, cols].reshape(bases * wide, 256)
            product = jnp.dot(design[...], panel, preferred_element_type=jnp.float32)
            dsend[:, cols] = product[mine:].astype(dsend.dtype)
            own[:, cols] = product[:mine]
        pair_copy(i).start()

    def pair_sum(i):
        pair_copy(i).wait_recv()
        own[:, slab(i)] = own[:, slab(i)] + drecv[:, slab(i)].astype(jnp.float32)

    def pass_on(step, i):
        for way in range(2):
            cols = way_cols(way, i)
            total = own_part(step, way, i)
            if step > 0:
                ring_copy(step - 1, way, i).wait_recv()
                total = total + rrecv[step - 1, :, cols].astype(jnp.float32)
            if step < pairs - 1:
                rsend[step, :, cols] = total.astype(rsend.dtype)
                ring_copy(step, way, i).start()
            else:
                done[:, cols] = total.astype(done.dtype)
        if step == pairs - 1:
            out_copy(i).start()

    @pl.loop(0, steps + LAGS[-1])
    def _(it):
        @pl.when(it < steps)
        def _():
            multiply(it)

        for step in range(pairs):
            lag = LAGS[step]

            @pl.when(jnp.logical_and(it >= lag, it < steps + lag))
            def _(step=step, lag=lag):
                if step == 0:
                    pair_sum(it - lag)
                pass_on(step, it - lag)

    for n in range(len(parts)):
        feature_copy(n).wait_send()

    @pl.loop(0, steps)
    def _(i):
        pair_copy(i).wait_send()
        for step in range(pairs - 1):
            for way in range(2):
                ring_copy(step, way, i).wait_send()
        out_copy(i).wait()


def predicted_block(features, hrf_filters, weights, n_chan):
    block, _ = features.shape
    bases, width, taps = hrf_filters.shape
    voxels = weights.shape[2]
    wide = up(width, LANES)
    steps = voxels // SLAB
    pairs = n_chan // 2
    sizes = (n_chan, bases, taps, width, wide, block, steps)
    hbm = pl.BlockSpec(memory_space=pl.ANY)
    dma = pltpu.SemaphoreType.DMA
    return pl.pallas_call(
        functools.partial(main_kernel, sizes),
        out_shape=jax.ShapeDtypeStruct((block, voxels), jnp.bfloat16),
        in_specs=[hbm, hbm, hbm],
        out_specs=hbm,
        scratch_shapes=[
            pltpu.VMEM((bases, wide, voxels), jnp.bfloat16),
            pltpu.VMEM((n_chan, block, wide), jnp.bfloat16),
            pltpu.VMEM((32 + n_chan * block, wide), jnp.float32),
            pltpu.VMEM((bases, taps, width), jnp.float32),
            pltpu.VMEM((bases, taps, wide), jnp.float32),
            pltpu.VMEM((n_chan * block, bases * wide), jnp.bfloat16),
            pltpu.VMEM((pairs * block, voxels), jnp.float32),
            pltpu.VMEM((pairs * block, voxels), jnp.bfloat16),
            pltpu.VMEM((pairs * block, voxels), jnp.bfloat16),
            pltpu.VMEM((pairs - 1, block, voxels), jnp.bfloat16),
            pltpu.VMEM((pairs - 1, block, voxels), jnp.bfloat16),
            pltpu.VMEM((block, voxels), jnp.bfloat16),
            dma((steps,)),
            dma,
            dma,
            dma((n_chan + 1,)),
            dma((n_chan + 1,)),
            dma((steps,)),
            dma((steps,)),
            dma((pairs - 1, 2, steps)),
            dma((pairs - 1, 2, steps)),
            dma((steps,)),
        ],
        compiler_params=pltpu.CompilerParams(
            collective_id=0, has_side_effects=True, vmem_limit_bytes=VMEM_LIMIT
        ),
        name="predict",
    )(features, hrf_filters.transpose(0, 2, 1), weights)


def route_kernel(owners, cap, vp_ref, table_ref, place_ref, dest_ref):
    groups = vp_ref.shape[0]
    parcel = vp_ref[...]
    high = parcel // LANES
    low = parcel - high * LANES
    owner_parts = []
    for h in range(SORT // LANES):
        lanes = slice(h * LANES, (h + 1) * LANES)
        found = jnp.full((groups, LANES), -1, jnp.int32)
        index = low[:, lanes]
        for row in range(table_ref.shape[0]):
            entries = jnp.broadcast_to(table_ref[row : row + 1, :], (groups, LANES))
            value = jnp.take_along_axis(entries, index, axis=1)
            found = jnp.where(high[:, lanes] == row, value, found)
        owner_parts.append(found)
    owner = jnp.concatenate(owner_parts, axis=1)

    def before(n):
        return (
            lax.broadcasted_iota(jnp.int32, (n, n), 0) < lax.broadcasted_iota(jnp.int32, (n, n), 1)
        )

    def ones(mask):
        return jnp.where(mask, 1.0, 0.0).astype(jnp.bfloat16)

    ahead = ones(before(SORT))
    lane = lax.broadcasted_iota(jnp.int32, (groups, LANES), 1)
    counts = jnp.zeros((groups, LANES), jnp.float32)
    ranks = []
    for o in range(owners):
        mask = jnp.where(owner == o, 1.0, 0.0)
        ranks.append(
            jnp.dot(mask.astype(jnp.bfloat16), ahead, preferred_element_type=jnp.float32)
        )
        counts = jnp.where(lane == o, jnp.sum(mask, axis=1, keepdims=True), counts)
    earlier = ones(
        lax.broadcasted_iota(jnp.int32, (groups, groups), 0)
        > lax.broadcasted_iota(jnp.int32, (groups, groups), 1)
    )
    start = jnp.dot(earlier, counts.astype(jnp.bfloat16), preferred_element_type=jnp.float32)
    start = start.astype(jnp.int32)
    counts = counts.astype(jnp.int32)
    first = start >> 3
    phase = start & 7
    tiles = jnp.where(counts > 0, (phase + counts + 7) >> 3, 0)
    tile_start = jnp.dot(
        tiles.astype(jnp.float32).astype(jnp.bfloat16), ones(before(LANES)),
        preferred_element_type=jnp.float32,
    ).astype(jnp.int32)

    def column(values, o):
        return jnp.sum(jnp.where(lane == o, values, 0), axis=1, keepdims=True)

    place = jnp.full((groups, SORT), -1, jnp.int32)
    dest = jnp.full((groups, LANES), owners * cap // TILE, jnp.int32)
    for o in range(owners):
        offset = column(tile_start * TILE + phase, o)
        place = jnp.where(owner == o, offset + ranks[o].astype(jnp.int32), place)
        low_tile = column(tile_start, o)
        top_tile = low_tile + column(tiles, o)
        spot = o * (cap // TILE) + column(first, o) + lane - low_tile
        dest = jnp.where(jnp.logical_and(lane >= low_tile, lane < top_tile), spot, dest)
    place_ref[...] = place
    dest_ref[...] = dest


def routes(voxel_parcel, parcel_owner, owners, cap):
    voxels = voxel_parcel.shape[0]
    groups = voxels // SORT
    rows = up(groups, 8)
    parcels = jnp.pad(
        voxel_parcel.reshape(groups, SORT), ((0, rows - groups), (0, 0)), constant_values=-1
    )
    entries = up(parcel_owner.shape[0], LANES)
    table = jnp.pad(parcel_owner, (0, entries - parcel_owner.shape[0])).reshape(-1, LANES)
    return pl.pallas_call(
        functools.partial(route_kernel, owners, cap),
        out_shape=(
            jax.ShapeDtypeStruct((rows, SORT), jnp.int32),
            jax.ShapeDtypeStruct((rows, LANES), jnp.int32),
        ),
        name="route",
    )(parcels, table)


def pack_kernel(groups, owners, dest_ref, place_ref, pred_hbm, out_ref, pred_ref, buf, loc, sem):
    block = pred_ref.shape[0]
    fetch = pltpu.make_async_copy(pred_hbm, pred_ref, sem)
    fetch.start()
    zero = jnp.zeros((64, LANES), jnp.float32)

    @pl.loop(0, buf.shape[0] // 64)
    def _(i):
        buf[pl.ds(pl.multiple_of(i * 64, 64), 64), :] = zero

    local_rows = LOCAL_TILES * TILE
    fetch.wait()

    @pl.loop(0, groups)
    def _(g):
        place = place_ref[pl.ds(g, 1), :]
        row = lax.broadcasted_iota(jnp.int32, (local_rows, SORT), 0)
        select = jnp.where(row == place, 1.0, 0.0).astype(jnp.bfloat16)
        part = pred_ref[:, pl.ds(pl.multiple_of(g * SORT, SORT), SORT)]
        twice = jnp.concatenate([part, part], axis=0)
        loc[...] = lax.dot_general(
            select, twice, (((1,), (1,)), ((), ())), preferred_element_type=jnp.float32
        )
        for base in range(0, LOCAL_TILES, GROUP):
            places = [
                pl.ds(pl.multiple_of(dest_ref[g, base + k] * TILE, TILE), TILE)
                for k in range(GROUP)
            ]
            held = [
                buf[spot, :] + loc[(base + k) * TILE : (base + k + 1) * TILE, :]
                for k, spot in enumerate(places)
            ]
            for spot, value in zip(places, held):
                buf[spot, :] = value

    pairs = owners // 2
    cap = out_ref.shape[2]
    left = lax.broadcasted_iota(jnp.int32, (cap, LANES), 1) < block
    unit = jnp.where(
        lax.broadcasted_iota(jnp.int32, (LANES, LANES), 0)
        == lax.broadcasted_iota(jnp.int32, (LANES, LANES), 1),
        1.0, 0.0,
    ).astype(jnp.bfloat16)

    @pl.loop(0, pairs)
    def _(p):
        first = buf[pl.ds(pl.multiple_of(p * cap, LANES), cap), :]
        second = buf[pl.ds(pl.multiple_of((pairs + p) * cap, LANES), cap), :]
        both = jnp.where(left, first, second).astype(jnp.bfloat16)
        turned = lax.dot_general(
            unit, both, (((1,), (1,)), ((), ())), preferred_element_type=jnp.float32
        ).astype(out_ref.dtype)
        out_ref[p] = turned[:block]
        out_ref[pairs + p] = turned[block:]


def packed_slots(predicted, place, dest, owners, cap):
    block, voxels = predicted.shape
    vmem = pl.BlockSpec(memory_space=pltpu.VMEM)
    return pl.pallas_call(
        functools.partial(pack_kernel, voxels // SORT, owners),
        out_shape=jax.ShapeDtypeStruct((owners, block, cap), jnp.bfloat16),
        in_specs=[
            pl.BlockSpec(memory_space=pltpu.SMEM), vmem, pl.BlockSpec(memory_space=pltpu.HBM)
        ],
        out_specs=vmem,
        scratch_shapes=[
            pltpu.VMEM((block, voxels), predicted.dtype),
            pltpu.VMEM((owners * cap + 64, LANES), jnp.float32),
            pltpu.VMEM((LOCAL_TILES * TILE, LANES), jnp.float32),
            pltpu.SemaphoreType.DMA,
        ],
        compiler_params=pltpu.CompilerParams(vmem_limit_bytes=16_000_000),
        name="pack",
    )(dest, place, predicted)


def exchange_kernel(n, in_ref, out_ref, local_sem, send_sem, recv_sem):
    me = lax.axis_index("vox")
    local = pltpu.make_async_copy(in_ref.at[me], out_ref.at[me], local_sem)
    local.start()
    barrier = pltpu.get_barrier_semaphore()
    for d in range(1, n):
        pl.semaphore_signal(
            barrier, inc=1, device_id={"vox": lax.rem(me + d, n)}, device_id_type=MESH
        )
    pl.semaphore_wait(barrier, n - 1)

    def block_copy(d):
        peer = lax.rem(me + d, n)
        return pltpu.make_async_remote_copy(
            src_ref=in_ref.at[peer], dst_ref=out_ref.at[me],
            send_sem=send_sem.at[d - 1], recv_sem=recv_sem.at[d - 1],
            device_id={"vox": peer}, device_id_type=MESH,
        )

    for d in range(1, n):
        block_copy(d).start()
    local.wait()
    for d in range(1, n):
        block_copy(d).wait()


def exchange(packed, n):
    dma = pltpu.SemaphoreType.DMA
    return pl.pallas_call(
        functools.partial(exchange_kernel, n),
        out_shape=jax.ShapeDtypeStruct(packed.shape, packed.dtype),
        in_specs=[pl.BlockSpec(memory_space=pl.ANY)],
        out_specs=pl.BlockSpec(memory_space=pl.ANY),
        scratch_shapes=[dma, dma((n - 1,)), dma((n - 1,))],
        compiler_params=pltpu.CompilerParams(
            collective_id=1, has_side_effects=True, vmem_limit_bytes=4_000_000
        ),
        name="exchange",
    )(packed)


def shards(features, hrf_filters, weights, voxel_parcel, parcel_owner):
    owners = lax.axis_size("vox")
    cap = 2 * voxel_parcel.shape[0] // owners
    place, dest = routes(voxel_parcel, parcel_owner, owners, cap)
    predicted = predicted_block(features, hrf_filters, weights, lax.axis_size("chan"))
    packed = packed_slots(predicted, place, dest, owners, cap)
    return exchange(packed, owners).transpose(0, 2, 1)


def solution(mesh):
    return jax.shard_map(
        shards,
        mesh=mesh,
        in_specs=(P("chan", None), P(None, "chan", None), P(None, "chan", "vox"), P("vox"), P()),
        out_specs=P("vox", None, "chan"),
        check_vma=False,
    )
```

```python
import functools

import jax
import jax.numpy as jnp
from jax import lax
from jax.experimental import pallas as pl
from jax.experimental.pallas import tpu as pltpu
from jax.sharding import PartitionSpec as P

MESH = pl.DeviceIdType.MESH
TAP_SPACING = 2
VMEM_LIMIT = 66_000_000
LANES = 128
SLAB = 512
SORT = 256
TILE = 8
LOCAL_TILES = 60
GROUP = 12
LAGS = (1, 3, 6, 10)


def up(value, multiple):
    return -(-value // multiple) * multiple


def ones(mask):
    return jnp.where(mask, 1.0, 0.0).astype(jnp.bfloat16)


def route(owners, cap, parcel_ref, table_ref, place_ref, dest_ref):
    rows = parcel_ref.shape[0]
    parcel = parcel_ref[...]
    high = parcel >> 7
    low = parcel & (LANES - 1)
    owner = jnp.zeros((rows, LANES), jnp.int32)
    for row in range(table_ref.shape[0]):
        line = jnp.broadcast_to(table_ref[row : row + 1, :], (rows, LANES))
        owner = jnp.where(high == row, jnp.take_along_axis(line, low, axis=1), owner)

    def iotas(n):
        shape = (n, n)
        return (
            lax.broadcasted_iota(jnp.int32, shape, 0), lax.broadcasted_iota(jnp.int32, shape, 1)
        )

    def dot(a, b):
        return jnp.dot(a, b, preferred_element_type=jnp.float32)

    first, second = iotas(LANES)
    ahead = ones(first < second)
    lane = lax.broadcasted_iota(jnp.int32, (rows, LANES), 1)
    counts = jnp.zeros((rows, LANES), jnp.float32)
    ranks = []
    for o in range(owners):
        mask = jnp.where(owner == o, 1.0, 0.0)
        ranks.append(dot(mask.astype(jnp.bfloat16), ahead))
        counts = jnp.where(lane == o, jnp.sum(mask, axis=1, keepdims=True), counts)
    counts = counts.astype(jnp.bfloat16)
    first, second = iotas(rows)
    start = dot(ones(second < first), counts).astype(jnp.int32)
    base = dot(ones((second >> 1) < (first >> 1)), counts).astype(jnp.int32)
    count = dot(ones((second >> 1) == (first >> 1)), counts).astype(jnp.int32)
    tile = base >> 3
    tiles = jnp.where(count > 0, ((base & 7) + count + 7) >> 3, 0)
    tile_start = dot(tiles.astype(jnp.float32).astype(jnp.bfloat16), ahead).astype(jnp.int32)

    def column(values, o):
        return jnp.sum(jnp.where(lane == o, values, 0), axis=1, keepdims=True)

    place = jnp.zeros((rows, LANES), jnp.int32)
    dest = jnp.full((rows, LANES), owners * cap // TILE, jnp.int32)
    offsets = (tile_start - tile) * TILE + start
    for o in range(owners):
        place = jnp.where(owner == o, column(offsets, o) + ranks[o].astype(jnp.int32), place)
        low_tile = column(tile_start, o)
        top_tile = low_tile + column(tiles, o)
        spot = o * (cap // TILE) + column(tile, o) + lane - low_tile
        dest = jnp.where(jnp.logical_and(lane >= low_tile, lane < top_tile), spot, dest)
    place_ref[...] = place
    dest_ref[...] = dest


def main_kernel(
    sizes,
    feat_ref, hrf_ref, w_ref, parcel_ref, table_ref, sorted_ref, dest_ref,
    wv, fe, series, hrf, coef, design, own, dsend, drecv, rsend, rrecv, place, ordered,
    w_sem, h_sem, f_local, f_send, f_recv, d_send, d_recv, r_send, r_recv, o_sem,
):
    n_chan, bases, taps, width, wide, block, steps, owners, cap = sizes
    pairs = n_chan // 2
    half = SLAB // 2
    me = lax.axis_index("chan")
    chip = me // 2
    core = lax.rem(me, 2)

    def device(away, flip):
        return lax.rem(chip + away, pairs) * 2 + (core if flip == 0 else 1 - core)

    shift = core * (wide - width)

    def weight_copy(i):
        cols = pl.ds(pl.multiple_of(i * SLAB, SLAB), SLAB)
        rows = pl.ds(pl.multiple_of(shift, 64), width)
        return pltpu.make_async_copy(w_ref.at[:, :, cols], wv.at[:, rows, cols], w_sem.at[i])

    def window(k):
        start = k * width - lax.rem(k, 2) * (wide - width)
        return pl.ds(pl.multiple_of(start, LANES), wide)

    local = pltpu.make_async_copy(feat_ref.at[:, window(me)], fe.at[me], f_local)
    local.start()
    taps_copy = pltpu.make_async_copy(hrf_ref, hrf, h_sem)
    taps_copy.start()

    barrier = pltpu.get_barrier_semaphore()
    for d in range(1, n_chan):
        pl.semaphore_signal(
            barrier, inc=1, device_id={"chan": lax.rem(me + d, n_chan)}, device_id_type=MESH
        )
    pl.semaphore_wait(barrier, n_chan - 1)

    parts = [(0, 1, 0, block)]
    parts += [(away, flip, 0, block) for away in (1, 3) for flip in (0, 1)]
    parts += [(2, flip, row, 32) for row in (32, 0) for flip in (0, 1)]

    def feature_copy(n):
        away, flip, row, rows = parts[n]
        peer = device(away, flip)
        return pltpu.make_async_remote_copy(
            src_ref=feat_ref.at[pl.ds(row, rows), window(peer)],
            dst_ref=fe.at[me, pl.ds(row, rows)],
            send_sem=f_send.at[n],
            recv_sem=f_recv.at[n],
            device_id={"chan": peer},
            device_id_type=MESH,
        )

    for n in range(len(parts)):
        feature_copy(n).start()

    @pl.loop(0, steps)
    def _(i):
        weight_copy(i).start()

    blank = pl.ds(pl.multiple_of((1 - core) * width, 64), wide - width)
    for b in range(bases):
        wv[b, blank, :] = jnp.zeros((wide - width, wv.shape[2]), wv.dtype)
    pad = 32
    series[:pad, :] = jnp.zeros((pad, wide), jnp.float32)

    def widen(source, row, rows):
        there = pl.ds(pl.multiple_of(pad + source * block + row, 32), rows)
        series[there, :] = fe[source, row : row + rows, :].astype(jnp.float32)

    def arrive(n):
        away, flip, row, rows = parts[n]
        feature_copy(n).wait_recv()
        widen(device(pairs - away, flip), row, rows)

    taps_copy.wait()
    coef[...] = jnp.zeros(coef.shape, coef.dtype)

    @pl.when(core == 0)
    def _():
        coef[:, :, :width] = hrf[...]

    @pl.when(core == 1)
    def _():
        coef[:, :, wide - width :] = hrf[...]

    local.wait()
    widen(me, 0, block)
    arrive(0)
    route(owners, cap, parcel_ref, table_ref, place, dest_ref)

    span = 32
    spans = block // span

    @pl.loop(0, n_chan * spans)
    def _(s):
        for when, some in ((spans, (1, 2, 3, 4)), (5 * spans, (5, 6)), (6 * spans, (7, 8))):

            @pl.when(s == when)
            def _(some=some):
                for n in some:
                    arrive(n)

        q = s // spans
        g = q // 3
        away = (1 + q) * (1 - g) * (2 - g) // 2 + (3 - q) * g * (2 - g) + (q - 2) * g * (g - 1) // 2
        r = lax.rem(chip * 2 + away + n_chan, n_chan)
        sub = lax.rem(s, spans)
        parity = lax.rem(r, 2)
        other = parity + core - 2 * parity * core
        row = (other * pairs + r // 2) * block + sub * span
        rows = pl.ds(pl.multiple_of(row, span), span)
        time = pl.multiple_of(r * block + sub * span, span)
        for lane in range(wide // LANES):
            lanes = slice(lane * LANES, (lane + 1) * LANES)
            past = series[pl.ds(time, pad + span), lanes]
            lagged = [past] + [pltpu.roll(past, TAP_SPACING * m, 0) for m in range(1, 4)]
            for b in range(bases):
                total = None
                for j in range(taps):
                    start = pad - TILE * (j // 4)
                    term = coef[b, j : j + 1, lanes] * lagged[j % 4][start : start + span]
                    total = term if total is None else total + term
                cols = slice(b * wide + lane * LANES, b * wide + (lane + 1) * LANES)
                design[rows, cols] = total.astype(design.dtype)

    mine = pairs * block

    def slab(i):
        return pl.ds(pl.multiple_of(i * SLAB, SLAB), SLAB)

    def way_cols(way, i):
        return pl.ds(pl.multiple_of(i * SLAB + way * half, half), half)

    def pair_copy(i):
        return pltpu.make_async_remote_copy(
            src_ref=dsend.at[:, slab(i)], dst_ref=drecv.at[:, slab(i)],
            send_sem=d_send.at[i], recv_sem=d_recv.at[i],
            device_id={"chan": device(0, 1)}, device_id_type=MESH,
        )

    def ring_copy(step, way, i):
        cols = way_cols(way, i)
        return pltpu.make_async_remote_copy(
            src_ref=rsend.at[step, :, cols], dst_ref=rrecv.at[step, :, cols],
            send_sem=r_send.at[step, way, i], recv_sem=r_recv.at[step, way, i],
            device_id={"chan": device((1, pairs - 1)[way], 0)}, device_id_type=MESH,
        )

    local_rows = LOCAL_TILES * TILE
    slab_groups = SLAB // SORT

    def out_copy(i):
        size = slab_groups * local_rows
        rows = pl.ds(pl.multiple_of(i * size, 16), size)
        return pltpu.make_async_copy(ordered.at[rows], sorted_ref.at[rows], o_sem.at[i])

    def sort_group(i, k, values):
        group = i * slab_groups + k
        spots = lax.broadcasted_iota(jnp.int32, (local_rows, LANES), 0)
        select = jnp.concatenate(
            [ones(spots == place[pl.ds(2 * group + h, 1), :]) for h in range(2)], axis=1
        )
        twice = jnp.concatenate([values, values], axis=0)
        rows = lax.dot_general(
            select, twice, (((1,), (1,)), ((), ())), preferred_element_type=jnp.float32
        )
        here = pl.ds(pl.multiple_of(group * local_rows, 16), local_rows)
        ordered[here, :] = rows.astype(ordered.dtype)

    def own_part(step, way, i):
        away = pairs - 1 - step if way == 0 else step + 1
        target = lax.rem(chip + away, pairs)
        return own[pl.ds(pl.multiple_of(target * block, block), block), way_cols(way, i)]

    def multiply(i):
        weight_copy(i).wait()
        for h in range(SLAB // 256):
            cols = pl.ds(pl.multiple_of(i * SLAB + h * 256, 256), 256)
            panel = wv[:, :, cols].reshape(bases * wide, 256)
            product = jnp.dot(design[...], panel, preferred_element_type=jnp.float32)
            dsend[:, cols] = product[mine:].astype(dsend.dtype)
            own[:, cols] = product[:mine]
        pair_copy(i).start()

    def pair_sum(i):
        pair_copy(i).wait_recv()
        own[:, slab(i)] = own[:, slab(i)] + drecv[:, slab(i)].astype(jnp.float32)

    def pass_on(step, i):
        for way in range(2):
            cols = way_cols(way, i)
            total = own_part(step, way, i)
            if step > 0:
                ring_copy(step - 1, way, i).wait_recv()
                total = total + rrecv[step - 1, :, cols].astype(jnp.float32)
            if step < pairs - 1:
                rsend[step, :, cols] = total.astype(rsend.dtype)
                ring_copy(step, way, i).start()
            else:
                sort_group(i, way, total.astype(jnp.bfloat16))
        if step == pairs - 1:
            out_copy(i).start()

    @pl.loop(0, steps + LAGS[-1])
    def _(it):
        @pl.when(it < steps)
        def _():
            multiply(it)

        for step in range(pairs):
            lag = LAGS[step]

            @pl.when(jnp.logical_and(it >= lag, it < steps + lag))
            def _(step=step, lag=lag):
                if step == 0:
                    pair_sum(it - lag)
                pass_on(step, it - lag)

    for n in range(len(parts)):
        feature_copy(n).wait_send()

    @pl.loop(0, steps)
    def _(i):
        pair_copy(i).wait_send()
        for step in range(pairs - 1):
            for way in range(2):
                ring_copy(step, way, i).wait_send()
        out_copy(i).wait()


def sorted_block(features, hrf_filters, weights, voxel_parcel, parcel_owner, n_chan, owners):
    block, _ = features.shape
    bases, width, taps = hrf_filters.shape
    voxels = weights.shape[2]
    wide = up(width, LANES)
    steps = voxels // SLAB
    pairs = n_chan // 2
    cap = 2 * voxels // owners
    sizes = (n_chan, bases, taps, width, wide, block, steps, owners, cap)
    parcels = voxel_parcel.reshape(-1, LANES)
    entries = up(parcel_owner.shape[0], LANES)
    table = jnp.pad(parcel_owner, (0, entries - parcel_owner.shape[0])).reshape(-1, LANES)
    sorted_rows = voxels // SORT * LOCAL_TILES * TILE
    hbm = pl.BlockSpec(memory_space=pl.ANY)
    vmem = pl.BlockSpec(memory_space=pltpu.VMEM)
    dma = pltpu.SemaphoreType.DMA
    return pl.pallas_call(
        functools.partial(main_kernel, sizes),
        out_shape=(
            jax.ShapeDtypeStruct((sorted_rows, 2 * block), jnp.bfloat16),
            jax.ShapeDtypeStruct(parcels.shape, jnp.int32),
        ),
        in_specs=[hbm, hbm, hbm, vmem, vmem],
        out_specs=(hbm, vmem),
        scratch_shapes=[
            pltpu.VMEM((bases, wide, voxels), jnp.bfloat16),
            pltpu.VMEM((n_chan, block, wide), jnp.bfloat16),
            pltpu.VMEM((32 + n_chan * block, wide), jnp.float32),
            pltpu.VMEM((bases, taps, width), jnp.float32),
            pltpu.VMEM((bases, taps, wide), jnp.float32),
            pltpu.VMEM((n_chan * block, bases * wide), jnp.bfloat16),
            pltpu.VMEM((pairs * block, voxels), jnp.float32),
            pltpu.VMEM((pairs * block, voxels), jnp.bfloat16),
            pltpu.VMEM((pairs * block, voxels), jnp.bfloat16),
            pltpu.VMEM((pairs - 1, block, voxels), jnp.bfloat16),
            pltpu.VMEM((pairs - 1, block, voxels), jnp.bfloat16),
            pltpu.VMEM(parcels.shape, jnp.int32),
            pltpu.VMEM((sorted_rows, 2 * block), jnp.bfloat16),
            dma((steps,)),
            dma,
            dma,
            dma((n_chan + 1,)),
            dma((n_chan + 1,)),
            dma((steps,)),
            dma((steps,)),
            dma((pairs - 1, 2, steps)),
            dma((pairs - 1, 2, steps)),
            dma((steps,)),
        ],
        compiler_params=pltpu.CompilerParams(
            collective_id=0, has_side_effects=True, vmem_limit_bytes=VMEM_LIMIT
        ),
        name="predict",
    )(features, hrf_filters.transpose(0, 2, 1), weights, parcels, table)


def pack_kernel(groups, owners, block, dest_ref, sorted_hbm, out_ref, held, buf, sem):
    local_rows = LOCAL_TILES * TILE
    parts = sem.shape[0]
    size = groups * local_rows // parts

    def fetch(k):
        here = pl.ds(k * size, size)
        return pltpu.make_async_copy(sorted_hbm.at[here], held.at[here], sem.at[k])

    for k in range(parts):
        fetch(k).start()
    zero = jnp.zeros((64, LANES), jnp.float32)

    @pl.loop(0, buf.shape[0] // 64)
    def _(i):
        buf[pl.ds(pl.multiple_of(i * 64, 64), 64), :] = zero

    for k in range(parts):
        fetch(k).wait()

        @pl.loop(k * groups // parts, (k + 1) * groups // parts)
        def _(g):
            for base in range(0, LOCAL_TILES, GROUP):
                start = pl.multiple_of(g * local_rows + base * TILE, 2 * TILE)
                added = held[pl.ds(start, GROUP * TILE), :].astype(jnp.float32)
                places = [
                    pl.ds(pl.multiple_of(dest_ref[2 * g, base + n] * TILE, TILE), TILE)
                    for n in range(GROUP)
                ]
                sums = [
                    buf[spot, :] + added[n * TILE : (n + 1) * TILE]
                    for n, spot in enumerate(places)
                ]
                for spot, value in zip(places, sums):
                    buf[spot, :] = value

    pairs = owners // 2
    cap = out_ref.shape[2]
    left = lax.broadcasted_iota(jnp.int32, (cap, LANES), 1) < block
    unit = jnp.where(
        lax.broadcasted_iota(jnp.int32, (LANES, LANES), 0)
        == lax.broadcasted_iota(jnp.int32, (LANES, LANES), 1),
        1.0, 0.0,
    ).astype(jnp.bfloat16)

    @pl.loop(0, pairs)
    def _(p):
        first = buf[pl.ds(pl.multiple_of(p * cap, LANES), cap), :]
        second = buf[pl.ds(pl.multiple_of((pairs + p) * cap, LANES), cap), :]
        both = jnp.where(left, first, second).astype(jnp.bfloat16)
        turned = lax.dot_general(
            unit, both, (((1,), (1,)), ((), ())), preferred_element_type=jnp.float32
        ).astype(out_ref.dtype)
        out_ref[p] = turned[:block]
        out_ref[pairs + p] = turned[block:]


def packed_slots(sorted_rows, dest, block, owners, cap):
    rows = sorted_rows.shape[0]
    groups = rows // (LOCAL_TILES * TILE)
    hbm = pl.BlockSpec(memory_space=pl.ANY)
    return pl.pallas_call(
        functools.partial(pack_kernel, groups, owners, block),
        out_shape=jax.ShapeDtypeStruct((owners, block, cap), jnp.bfloat16),
        in_specs=[pl.BlockSpec(memory_space=pltpu.SMEM), hbm],
        out_specs=pl.BlockSpec(memory_space=pltpu.VMEM),
        scratch_shapes=[
            pltpu.VMEM(sorted_rows.shape, sorted_rows.dtype),
            pltpu.VMEM((owners * cap + 64, LANES), jnp.float32),
            pltpu.SemaphoreType.DMA((4,)),
        ],
        compiler_params=pltpu.CompilerParams(vmem_limit_bytes=60_000_000),
        name="pack",
    )(dest, sorted_rows)


def exchange_kernel(n, in_ref, out_ref, local_sem, send_sem, recv_sem):
    me = lax.axis_index("vox")
    side = 4
    local = pltpu.make_async_copy(in_ref.at[me], out_ref.at[me], local_sem)
    local.start()
    barrier = pltpu.get_barrier_semaphore()
    for d in range(1, n):
        pl.semaphore_signal(
            barrier, inc=1, device_id={"vox": lax.rem(me + d, n)}, device_id_type=MESH
        )
    pl.semaphore_wait(barrier, n - 1)

    def block_copy(d):
        up_z, up_y = divmod(d, side)
        peer = lax.rem(me // side + up_z, n // side) * side + lax.rem(me + up_y, side)
        return pltpu.make_async_remote_copy(
            src_ref=in_ref.at[peer], dst_ref=out_ref.at[me],
            send_sem=send_sem.at[d - 1], recv_sem=recv_sem.at[d - 1],
            device_id={"vox": peer}, device_id_type=MESH,
        )

    apart = {d: sum(min(k, side - k) for k in divmod(d, side)) for d in range(1, n)}
    for d in sorted(apart, key=lambda d: -apart[d]):
        block_copy(d).start()
    local.wait()
    for d in range(1, n):
        block_copy(d).wait()


def exchange(packed, n):
    dma = pltpu.SemaphoreType.DMA
    return pl.pallas_call(
        functools.partial(exchange_kernel, n),
        out_shape=jax.ShapeDtypeStruct(packed.shape, packed.dtype),
        in_specs=[pl.BlockSpec(memory_space=pl.ANY)],
        out_specs=pl.BlockSpec(memory_space=pl.ANY),
        scratch_shapes=[dma, dma((n - 1,)), dma((n - 1,))],
        compiler_params=pltpu.CompilerParams(
            collective_id=1, has_side_effects=True, vmem_limit_bytes=60_000_000
        ),
        name="exchange",
    )(packed)


def shards(features, hrf_filters, weights, voxel_parcel, parcel_owner):
    owners = lax.axis_size("vox")
    block = features.shape[0]
    cap = 2 * voxel_parcel.shape[0] // owners
    sorted_rows, dest = sorted_block(
        features, hrf_filters, weights, voxel_parcel, parcel_owner, lax.axis_size("chan"), owners
    )
    packed = packed_slots(sorted_rows, dest, block, owners, cap)
    return exchange(packed, owners).transpose(0, 2, 1)


def solution(mesh):
    return jax.shard_map(
        shards,
        mesh=mesh,
        in_specs=(P("chan", None), P(None, "chan", None), P(None, "chan", "vox"), P("vox"), P()),
        out_specs=P("vox", None, "chan"),
        check_vma=False,
    )
```

```python
import functools

import jax
import jax.numpy as jnp
from jax import lax
from jax.experimental import pallas as pl
from jax.experimental.pallas import tpu as pltpu
from jax.sharding import PartitionSpec as P

MESH = pl.DeviceIdType.MESH
TAP_SPACING = 2
VMEM_LIMIT = 66_000_000
LANES = 128
SLAB = 512
SORT = 256
TILE = 8
LOCAL_TILES = 60
LAGS = (1, 3, 6, 10)


def up(value, multiple):
    return -(-value // multiple) * multiple


def ones(mask):
    return jnp.where(mask, 1.0, 0.0).astype(jnp.bfloat16)


def route(owners, cap, parcel_ref, table_ref, place_ref, lists_ref):
    rows = parcel_ref.shape[0]
    parcel = parcel_ref[...]
    high = parcel >> 7
    low = parcel & (LANES - 1)
    owner = jnp.zeros((rows, LANES), jnp.int32)
    entries = table_ref.shape[0]
    for row in range(up(entries, LANES) // LANES):
        line = table_ref[pl.ds(row * LANES, min(LANES, entries - row * LANES))][None, :]
        if line.shape[1] < LANES:
            rest = jnp.zeros((1, LANES - line.shape[1]), jnp.int32)
            line = jnp.concatenate([line, rest], axis=1)
        line = jnp.broadcast_to(line, (rows, LANES))
        owner = jnp.where(high == row, jnp.take_along_axis(line, low, axis=1), owner)

    def iotas(n):
        shape = (n, n)
        return (
            lax.broadcasted_iota(jnp.int32, shape, 0), lax.broadcasted_iota(jnp.int32, shape, 1)
        )

    def dot(a, b):
        return jnp.dot(a, b, preferred_element_type=jnp.float32)

    first, second = iotas(LANES)
    ahead = ones(first < second)
    lane = lax.broadcasted_iota(jnp.int32, (rows, LANES), 1)
    counts = jnp.zeros((rows, LANES), jnp.float32)
    ranks = []
    for o in range(owners):
        mask = jnp.where(owner == o, 1.0, 0.0)
        ranks.append(dot(mask.astype(jnp.bfloat16), ahead))
        counts = jnp.where(lane == o, jnp.sum(mask, axis=1, keepdims=True), counts)
    counts = counts.astype(jnp.bfloat16)
    first, second = iotas(rows)
    start = dot(ones(second < first), counts).astype(jnp.int32)
    base = dot(ones((second >> 1) < (first >> 1)), counts).astype(jnp.int32)
    before = dot(ones((second >> 1) < (first >> 1) - 1), counts).astype(jnp.int32)
    count = dot(ones((second >> 1) == (first >> 1)), counts).astype(jnp.int32)
    tile = base >> 3
    tiles = jnp.where(count > 0, ((base & 7) + count + 7) >> 3, 0)
    tile_start = dot(tiles.astype(jnp.float32).astype(jnp.bfloat16), ahead).astype(jnp.int32)

    def column(values, o):
        return jnp.sum(jnp.where(lane == o, values, 0), axis=1, keepdims=True)

    place = jnp.zeros((rows, LANES), jnp.int32)
    offsets = (tile_start - tile) * TILE + start
    row = lax.broadcasted_iota(jnp.int32, (rows, LANES), 0)
    whole = (row & 1) == 0
    empty = rows // 2 * LOCAL_TILES
    for o in range(owners):
        place = jnp.where(owner == o, column(offsets, o) + ranks[o].astype(jnp.int32), place)
        low = column(tile, o)
        slot = lane * TILE - column(base, o)
        opens = jnp.logical_and(whole, jnp.logical_and(slot >= 0, slot < column(count, o)))
        sources = (row >> 1) * LOCAL_TILES + column(tile_start, o) + lane - low - empty

        def total(mask, values):
            picked = jnp.where(mask, values.astype(jnp.float32), 0.0)
            return jnp.sum(picked, axis=0, keepdims=True).astype(jnp.int32)

        single = jnp.ones((rows, LANES), jnp.int32)
        lists_ref[o : o + 1, :] = jnp.clip(total(opens, sources) + empty, 0, empty)
        starts = total(jnp.logical_and(whole, low == lane), single)
        so_far = total(jnp.logical_and(whole, low <= lane), single)
        so_far = jnp.clip(so_far, 0, rows // 2)
        lists_ref[owners + o : owners + o + 1, :] = jnp.where(starts > 0, so_far, 0) * owners + o
    inside = jnp.logical_and((base & 7) != 0, count > 0)
    added = jnp.where(inside, (row >> 1) * LOCAL_TILES + tile_start, empty)
    lists_ref[2 * owners : 2 * owners + rows, :] = jnp.clip(added, 0, empty)
    lists_ref[2 * owners + rows :, :] = jnp.where(tile == before >> 3, 1, 0)
    place_ref[...] = place


def main_kernel(
    sizes,
    feat_ref, hrf_ref, w_ref, parcel_ref, table_ref, out_ref,
    wv, fe, series, hrf, coef, design, own, dsend, drecv, rsend, rrecv,
    place, lists, lists_s, ordered, sums, gathered, packed,
    w_sem, h_sem, f_local, f_send, f_recv, d_send, d_recv, r_send, r_recv, s_sem, x_local, x_send, x_recv,
):
    n_chan, bases, taps, width, wide, block, steps, owners, cap = sizes
    pairs = n_chan // 2
    half = SLAB // 2
    me = lax.axis_index("chan")
    here = lax.axis_index("vox")
    chip = me // 2
    core = lax.rem(me, 2)

    def device(away, flip):
        return lax.rem(chip + away, pairs) * 2 + (core if flip == 0 else 1 - core)

    shift = core * (wide - width)

    def weight_copy(i):
        cols = pl.ds(pl.multiple_of(i * SLAB, SLAB), SLAB)
        rows = pl.ds(pl.multiple_of(shift, 64), width)
        return pltpu.make_async_copy(w_ref.at[:, :, cols], wv.at[:, rows, cols], w_sem.at[i])

    def window(k):
        start = k * width - lax.rem(k, 2) * (wide - width)
        return pl.ds(pl.multiple_of(start, LANES), wide)

    local = pltpu.make_async_copy(feat_ref.at[:, window(me)], fe.at[me], f_local)
    local.start()
    taps_copy = pltpu.make_async_copy(hrf_ref, hrf, h_sem)
    taps_copy.start()

    barrier = pltpu.get_barrier_semaphore()
    for d in range(1, n_chan):
        pl.semaphore_signal(
            barrier, inc=1, device_id={"chan": lax.rem(me + d, n_chan)}, device_id_type=MESH
        )
    for d in range(1, owners):
        pl.semaphore_signal(
            barrier, inc=1, device_id={"vox": lax.rem(here + d, owners)}, device_id_type=MESH
        )
    pl.semaphore_wait(barrier, n_chan + owners - 2)

    parts = [(0, 1, 0, block)]
    parts += [(away, flip, 0, block) for away in (1, 3) for flip in (0, 1)]
    parts += [(2, flip, row, 32) for row in (32, 0) for flip in (0, 1)]

    def feature_copy(n):
        away, flip, row, rows = parts[n]
        peer = device(away, flip)
        return pltpu.make_async_remote_copy(
            src_ref=feat_ref.at[pl.ds(row, rows), window(peer)],
            dst_ref=fe.at[me, pl.ds(row, rows)],
            send_sem=f_send.at[n],
            recv_sem=f_recv.at[n],
            device_id={"chan": peer},
            device_id_type=MESH,
        )

    for n in range(len(parts)):
        feature_copy(n).start()

    @pl.loop(0, steps)
    def _(i):
        weight_copy(i).start()

    blank = pl.ds(pl.multiple_of((1 - core) * width, 64), wide - width)
    for b in range(bases):
        wv[b, blank, :] = jnp.zeros((wide - width, wv.shape[2]), wv.dtype)
    pad = 32
    series[:pad, :] = jnp.zeros((pad, wide), jnp.float32)

    def widen(source, row, rows):
        there = pl.ds(pl.multiple_of(pad + source * block + row, 32), rows)
        series[there, :] = fe[source, row : row + rows, :].astype(jnp.float32)

    def arrive(n):
        away, flip, row, rows = parts[n]
        feature_copy(n).wait_recv()
        widen(device(pairs - away, flip), row, rows)

    taps_copy.wait()
    coef[...] = jnp.zeros(coef.shape, coef.dtype)

    @pl.when(core == 0)
    def _():
        coef[:, :, :width] = hrf[...]

    @pl.when(core == 1)
    def _():
        coef[:, :, wide - width :] = hrf[...]

    local.wait()
    widen(me, 0, block)
    arrive(0)
    route(owners, cap, parcel_ref, table_ref, place, lists)
    to_scalars = pltpu.make_async_copy(lists, lists_s, s_sem)
    to_scalars.start()
    ordered[ordered.shape[0] - 1] = jnp.zeros((TILE, LANES), jnp.float32)
    sums[:owners] = jnp.zeros((owners, TILE, LANES), jnp.float32)

    span = 32
    spans = block // span

    @pl.loop(0, n_chan * spans)
    def _(s):
        for when, some in ((spans, (1, 2, 3, 4)), (5 * spans, (5, 6)), (6 * spans, (7, 8))):

            @pl.when(s == when)
            def _(some=some):
                for n in some:
                    arrive(n)

        q = s // spans
        g = q // 3
        away = (1 + q) * (1 - g) * (2 - g) // 2 + (3 - q) * g * (2 - g) + (q - 2) * g * (g - 1) // 2
        r = lax.rem(chip * 2 + away + n_chan, n_chan)
        sub = lax.rem(s, spans)
        parity = lax.rem(r, 2)
        other = parity + core - 2 * parity * core
        row = (other * pairs + r // 2) * block + sub * span
        rows = pl.ds(pl.multiple_of(row, span), span)
        time = pl.multiple_of(r * block + sub * span, span)
        for lane in range(wide // LANES):
            lanes = slice(lane * LANES, (lane + 1) * LANES)
            past = series[pl.ds(time, pad + span), lanes]
            lagged = [past] + [pltpu.roll(past, TAP_SPACING * m, 0) for m in range(1, 4)]
            for b in range(bases):
                total = None
                for j in range(taps):
                    start = pad - TILE * (j // 4)
                    term = coef[b, j : j + 1, lanes] * lagged[j % 4][start : start + span]
                    total = term if total is None else total + term
                cols = slice(b * wide + lane * LANES, b * wide + (lane + 1) * LANES)
                design[rows, cols] = total.astype(design.dtype)

    mine = pairs * block

    def slab(i):
        return pl.ds(pl.multiple_of(i * SLAB, SLAB), SLAB)

    def way_cols(way, i):
        return pl.ds(pl.multiple_of(i * SLAB + way * half, half), half)

    def pair_copy(i):
        return pltpu.make_async_remote_copy(
            src_ref=dsend.at[:, slab(i)], dst_ref=drecv.at[:, slab(i)],
            send_sem=d_send.at[i], recv_sem=d_recv.at[i],
            device_id={"chan": device(0, 1)}, device_id_type=MESH,
        )

    def ring_copy(step, way, i):
        cols = way_cols(way, i)
        return pltpu.make_async_remote_copy(
            src_ref=rsend.at[step, :, cols], dst_ref=rrecv.at[step, :, cols],
            send_sem=r_send.at[step, way, i], recv_sem=r_recv.at[step, way, i],
            device_id={"chan": device((1, pairs - 1)[way], 0)}, device_id_type=MESH,
        )

    local_rows = LOCAL_TILES * TILE
    slab_groups = SLAB // SORT

    def sort_group(i, k, values):
        group = i * slab_groups + k
        spots = lax.broadcasted_iota(jnp.int32, (local_rows, LANES), 0)
        select = jnp.concatenate(
            [ones(spots == place[pl.ds(2 * group + h, 1), :]) for h in range(2)], axis=1
        )
        twice = jnp.concatenate([values, values], axis=0)
        rows = lax.dot_general(
            select, twice, (((1,), (1,)), ((), ())), preferred_element_type=jnp.float32
        )
        ordered[pl.ds(group * LOCAL_TILES, LOCAL_TILES)] = rows.reshape(LOCAL_TILES, TILE, LANES)
        added = lists_s.at[pl.ds(2 * owners + 2 * group, 1)]
        goes_on = lists_s.at[pl.ds(2 * owners + place.shape[0] + 2 * group, 1)]
        past = sums.at[pl.ds(group * owners, owners)]
        now = sums.at[pl.ds((group + 1) * owners, owners)]
        for o in range(owners):
            now[o] = past[o] * goes_on[0, o].astype(jnp.float32) + ordered[added[0, o]]

    def own_part(step, way, i):
        away = pairs - 1 - step if way == 0 else step + 1
        target = lax.rem(chip + away, pairs)
        return own[pl.ds(pl.multiple_of(target * block, block), block), way_cols(way, i)]

    def multiply(i):
        weight_copy(i).wait()
        for h in range(SLAB // 256):
            cols = pl.ds(pl.multiple_of(i * SLAB + h * 256, 256), 256)
            panel = wv[:, :, cols].reshape(bases * wide, 256)
            product = jnp.dot(design[...], panel, preferred_element_type=jnp.float32)
            dsend[:, cols] = product[mine:].astype(dsend.dtype)
            own[:, cols] = product[:mine]
        pair_copy(i).start()

    def pair_sum(i):
        pair_copy(i).wait_recv()
        own[:, slab(i)] = own[:, slab(i)] + drecv[:, slab(i)].astype(jnp.float32)

    def pass_on(step, i):
        for way in range(2):
            cols = way_cols(way, i)
            total = own_part(step, way, i)
            if step > 0:
                ring_copy(step - 1, way, i).wait_recv()
                total = total + rrecv[step - 1, :, cols].astype(jnp.float32)
            if step < pairs - 1:
                rsend[step, :, cols] = total.astype(rsend.dtype)
                ring_copy(step, way, i).start()
            else:
                sort_group(i, way, total.astype(jnp.bfloat16))

    to_scalars.wait()

    @pl.loop(0, steps + LAGS[-1])
    def _(it):
        @pl.when(it < steps)
        def _():
            multiply(it)

        for step in range(pairs):
            lag = LAGS[step]

            @pl.when(jnp.logical_and(it >= lag, it < steps + lag))
            def _(step=step, lag=lag):
                if step == 0:
                    pair_sum(it - lag)
                pass_on(step, it - lag)

    side = 4
    unit = ones(
        lax.broadcasted_iota(jnp.int32, (block, LANES), 0)
        == lax.broadcasted_iota(jnp.int32, (block, LANES), 1)
    )

    def fill(owner):
        unroll = 8
        opens = lists_s.at[pl.ds(owner, 1)]
        rest = lists_s.at[pl.ds(owners + owner, 1)]

        @pl.loop(0, cap // TILE // unroll)
        def _(s):
            for u in range(unroll):
                tile = s * unroll + u
                gathered[pl.ds(pl.multiple_of(tile * TILE, TILE), TILE), :] = (
                    ordered[opens[0, tile]] + sums[rest[0, tile]]
                )

        packed[owner] = lax.dot_general(
            unit, gathered[...].astype(jnp.bfloat16), (((1,), (1,)), ((), ())),
            preferred_element_type=jnp.float32,
        ).astype(packed.dtype)

    def peer_of(d):
        up_z, up_y = divmod(d, side)
        return lax.rem(here // side + up_z, owners // side) * side + lax.rem(here + up_y, side)

    def block_copy(d):
        return pltpu.make_async_remote_copy(
            src_ref=packed.at[peer_of(d)], dst_ref=out_ref.at[here],
            send_sem=x_send.at[d - 1], recv_sem=x_recv.at[d - 1],
            device_id={"vox": peer_of(d)}, device_id_type=MESH,
        )

    apart = {d: sum(min(k, side - k) for k in divmod(d, side)) for d in range(1, owners)}
    for d in sorted(apart, key=lambda d: -apart[d]):
        fill(peer_of(d))
        block_copy(d).start()
    fill(here)
    kept = pltpu.make_async_copy(packed.at[here], out_ref.at[here], x_local)
    kept.start()

    for n in range(len(parts)):
        feature_copy(n).wait_send()

    @pl.loop(0, steps)
    def _(i):
        pair_copy(i).wait_send()
        for step in range(pairs - 1):
            for way in range(2):
                ring_copy(step, way, i).wait_send()

    kept.wait()
    for d in range(1, owners):
        block_copy(d).wait()


def owned_block(features, hrf_filters, weights, voxel_parcel, parcel_owner, n_chan, owners):
    block, _ = features.shape
    bases, width, taps = hrf_filters.shape
    voxels = weights.shape[2]
    wide = up(width, LANES)
    steps = voxels // SLAB
    pairs = n_chan // 2
    cap = 2 * voxels // owners
    sizes = (n_chan, bases, taps, width, wide, block, steps, owners, cap)
    parcels = voxel_parcel.reshape(-1, LANES)
    sorted_tiles = voxels // SORT * LOCAL_TILES
    hbm = pl.BlockSpec(memory_space=pl.ANY)
    vmem = pl.BlockSpec(memory_space=pltpu.VMEM)
    dma = pltpu.SemaphoreType.DMA
    return pl.pallas_call(
        functools.partial(main_kernel, sizes),
        out_shape=jax.ShapeDtypeStruct((owners, block, cap), jnp.bfloat16),
        in_specs=[hbm, hbm, hbm, vmem, vmem],
        out_specs=hbm,
        scratch_shapes=[
            pltpu.VMEM((bases, wide, voxels), jnp.bfloat16),
            pltpu.VMEM((n_chan, block, wide), jnp.bfloat16),
            pltpu.VMEM((32 + n_chan * block, wide), jnp.float32),
            pltpu.VMEM((bases, taps, width), jnp.float32),
            pltpu.VMEM((bases, taps, wide), jnp.float32),
            pltpu.VMEM((n_chan * block, bases * wide), jnp.bfloat16),
            pltpu.VMEM((pairs * block, voxels), jnp.float32),
            pltpu.VMEM((pairs * block, voxels), jnp.bfloat16),
            pltpu.VMEM((pairs * block, voxels), jnp.bfloat16),
            pltpu.VMEM((pairs - 1, block, voxels), jnp.bfloat16),
            pltpu.VMEM((pairs - 1, block, voxels), jnp.bfloat16),
            pltpu.VMEM(parcels.shape, jnp.int32),
            pltpu.VMEM((2 * owners + 2 * parcels.shape[0], LANES), jnp.int32),
            pltpu.SMEM((2 * owners + 2 * parcels.shape[0], LANES), jnp.int32),
            pltpu.VMEM((sorted_tiles + 1, TILE, LANES), jnp.float32),
            pltpu.VMEM(((voxels // SORT + 1) * owners, TILE, LANES), jnp.float32),
            pltpu.VMEM((cap, LANES), jnp.float32),
            pltpu.VMEM((owners, block, cap), jnp.bfloat16),
            dma((steps,)),
            dma,
            dma,
            dma((n_chan + 1,)),
            dma((n_chan + 1,)),
            dma((steps,)),
            dma((steps,)),
            dma((pairs - 1, 2, steps)),
            dma((pairs - 1, 2, steps)),
            dma,
            dma,
            dma((owners - 1,)),
            dma((owners - 1,)),
        ],
        compiler_params=pltpu.CompilerParams(
            collective_id=0, has_side_effects=True, vmem_limit_bytes=VMEM_LIMIT
        ),
        name="predict",
    )(features, hrf_filters.transpose(0, 2, 1), weights, parcels, parcel_owner)


def shards(features, hrf_filters, weights, voxel_parcel, parcel_owner):
    owners = lax.axis_size("vox")
    owned = owned_block(
        features, hrf_filters, weights, voxel_parcel, parcel_owner, lax.axis_size("chan"), owners
    )
    return owned.transpose(0, 2, 1)


def solution(mesh):
    return jax.shard_map(
        shards,
        mesh=mesh,
        in_specs=(P("chan", None), P(None, "chan", None), P(None, "chan", "vox"), P("vox"), P()),
        out_specs=P("vox", None, "chan"),
        check_vma=False,
    )
```

```python
import functools

import jax
import jax.numpy as jnp
from jax import lax
from jax.experimental import pallas as pl
from jax.experimental.pallas import tpu as pltpu
from jax.sharding import PartitionSpec as P

MESH = pl.DeviceIdType.MESH
TAP_SPACING = 2
VMEM_LIMIT = 60_000_000
LANES = 128
SLAB = 512
SORT = 256
TILE = 8
LOCAL_TILES = 60
LAGS = (1, 3, 6, 10)


def up(value, multiple):
    return -(-value // multiple) * multiple


def ones(mask):
    return jnp.where(mask, 1.0, 0.0).astype(jnp.bfloat16)


def route(owners, cap, parcel_ref, table_ref, place_ref, lists_ref):
    rows = parcel_ref.shape[0]
    parcel = parcel_ref[...]
    high = parcel >> 7
    low = parcel & (LANES - 1)
    owner = jnp.zeros((rows, LANES), jnp.int32)
    entries = table_ref.shape[0]
    for row in range(up(entries, LANES) // LANES):
        line = table_ref[pl.ds(row * LANES, min(LANES, entries - row * LANES))][None, :]
        if line.shape[1] < LANES:
            rest = jnp.zeros((1, LANES - line.shape[1]), jnp.int32)
            line = jnp.concatenate([line, rest], axis=1)
        line = jnp.broadcast_to(line, (rows, LANES))
        owner = jnp.where(high == row, jnp.take_along_axis(line, low, axis=1), owner)

    def iotas(n):
        shape = (n, n)
        return (
            lax.broadcasted_iota(jnp.int32, shape, 0), lax.broadcasted_iota(jnp.int32, shape, 1)
        )

    def dot(a, b):
        return jnp.dot(a, b, preferred_element_type=jnp.float32)

    first, second = iotas(LANES)
    ahead = ones(first < second)
    lane = lax.broadcasted_iota(jnp.int32, (rows, LANES), 1)
    counts = jnp.zeros((rows, LANES), jnp.float32)
    ranks = []
    for o in range(owners):
        mask = jnp.where(owner == o, 1.0, 0.0)
        ranks.append(dot(mask.astype(jnp.bfloat16), ahead))
        counts = jnp.where(lane == o, jnp.sum(mask, axis=1, keepdims=True), counts)
    counts = counts.astype(jnp.bfloat16)
    first, second = iotas(rows)
    start = dot(ones(second < first), counts).astype(jnp.int32)
    base = dot(ones((second >> 1) < (first >> 1)), counts).astype(jnp.int32)
    before = dot(ones((second >> 1) < (first >> 1) - 1), counts).astype(jnp.int32)
    count = dot(ones((second >> 1) == (first >> 1)), counts).astype(jnp.int32)
    tile = base >> 3
    tiles = jnp.where(count > 0, ((base & 7) + count + 7) >> 3, 0)
    tile_start = dot(tiles.astype(jnp.float32).astype(jnp.bfloat16), ahead).astype(jnp.int32)

    def column(values, o):
        return jnp.sum(jnp.where(lane == o, values, 0), axis=1, keepdims=True)

    place = jnp.zeros((rows, LANES), jnp.int32)
    offsets = (tile_start - tile) * TILE + start
    row = lax.broadcasted_iota(jnp.int32, (rows, LANES), 0)
    whole = (row & 1) == 0
    empty = rows // 2 * LOCAL_TILES
    for o in range(owners):
        place = jnp.where(owner == o, column(offsets, o) + ranks[o].astype(jnp.int32), place)
        low = column(tile, o)
        slot = lane * TILE - column(base, o)
        opens = jnp.logical_and(whole, jnp.logical_and(slot >= 0, slot < column(count, o)))
        sources = (row >> 1) * LOCAL_TILES + column(tile_start, o) + lane - low - empty

        def total(mask, values):
            picked = jnp.where(mask, values.astype(jnp.float32), 0.0)
            return jnp.sum(picked, axis=0, keepdims=True).astype(jnp.int32)

        single = jnp.ones((rows, LANES), jnp.int32)
        lists_ref[o : o + 1, :] = jnp.clip(total(opens, sources) + empty, 0, empty)
        starts = total(jnp.logical_and(whole, low == lane), single)
        so_far = total(jnp.logical_and(whole, low <= lane), single)
        so_far = jnp.clip(so_far, 0, rows // 2)
        lists_ref[owners + o : owners + o + 1, :] = jnp.where(starts > 0, so_far, 0) * owners + o
    inside = jnp.logical_and((base & 7) != 0, count > 0)
    added = jnp.where(inside, (row >> 1) * LOCAL_TILES + tile_start, empty)
    lists_ref[2 * owners : 2 * owners + rows, :] = jnp.clip(added, 0, empty)
    lists_ref[2 * owners + rows :, :] = jnp.where(tile == before >> 3, 1, 0)
    place_ref[...] = place


def main_kernel(
    sizes,
    feat_ref, hrf_ref, w_ref, parcel_ref, table_ref, out_ref,
    wv, fe, series, hrf, coef, design, own, dsend, drecv, rsend, rrecv,
    place, lists, lists_s, ordered, sums, gathered, packed,
    w_sem, h_sem, f_local, f_send, f_recv, d_send, d_recv, r_send, r_recv, s_sem, x_local, x_send, x_recv,
):
    n_chan, bases, taps, width, wide, block, steps, owners, cap = sizes
    pairs = n_chan // 2
    half = SLAB // 2
    me = lax.axis_index("chan")
    here = lax.axis_index("vox")
    chip = me // 2
    core = lax.rem(me, 2)

    def device(away, flip):
        return lax.rem(chip + away, pairs) * 2 + (core if flip == 0 else 1 - core)

    shift = core * (wide - width)

    def weight_copy(i):
        cols = pl.ds(pl.multiple_of(i * SLAB, SLAB), SLAB)
        rows = pl.ds(pl.multiple_of(shift, 64), width)
        return pltpu.make_async_copy(w_ref.at[:, :, cols], wv.at[:, rows, cols], w_sem.at[i])

    def window(k):
        start = k * width - lax.rem(k, 2) * (wide - width)
        return pl.ds(pl.multiple_of(start, LANES), wide)

    local = pltpu.make_async_copy(feat_ref.at[:, window(me)], fe.at[me], f_local)
    local.start()
    taps_copy = pltpu.make_async_copy(hrf_ref, hrf, h_sem)
    taps_copy.start()

    barrier = pltpu.get_barrier_semaphore()
    for d in range(1, n_chan):
        pl.semaphore_signal(
            barrier, inc=1, device_id={"chan": lax.rem(me + d, n_chan)}, device_id_type=MESH
        )
    for d in range(1, owners):
        pl.semaphore_signal(
            barrier, inc=1, device_id={"vox": lax.rem(here + d, owners)}, device_id_type=MESH
        )
    pl.semaphore_wait(barrier, n_chan + owners - 2)

    parts = [(0, 1, 0, block)]
    parts += [(away, flip, 0, block) for away in (1, 3) for flip in (0, 1)]
    parts += [(2, flip, row, 32) for row in (32, 0) for flip in (0, 1)]

    def feature_copy(n):
        away, flip, row, rows = parts[n]
        peer = device(away, flip)
        return pltpu.make_async_remote_copy(
            src_ref=feat_ref.at[pl.ds(row, rows), window(peer)],
            dst_ref=fe.at[me, pl.ds(row, rows)],
            send_sem=f_send.at[n],
            recv_sem=f_recv.at[n],
            device_id={"chan": peer},
            device_id_type=MESH,
        )

    for n in range(len(parts)):
        feature_copy(n).start()

    @pl.loop(0, steps)
    def _(i):
        weight_copy(i).start()

    blank = pl.ds(pl.multiple_of((1 - core) * width, 64), wide - width)
    for b in range(bases):
        wv[b, blank, :] = jnp.zeros((wide - width, wv.shape[2]), wv.dtype)
    pad = 32
    series[:pad, :] = jnp.zeros((pad, wide), jnp.float32)

    def widen(source, row, rows):
        there = pl.ds(pl.multiple_of(pad + source * block + row, 32), rows)
        series[there, :] = fe[source, row : row + rows, :].astype(jnp.float32)

    def arrive(n):
        away, flip, row, rows = parts[n]
        feature_copy(n).wait_recv()
        widen(device(pairs - away, flip), row, rows)

    taps_copy.wait()
    coef[...] = jnp.zeros(coef.shape, coef.dtype)

    @pl.when(core == 0)
    def _():
        coef[:, :, :width] = hrf[...]

    @pl.when(core == 1)
    def _():
        coef[:, :, wide - width :] = hrf[...]

    local.wait()
    widen(me, 0, block)
    arrive(0)
    route(owners, cap, parcel_ref, table_ref, place, lists)
    to_scalars = pltpu.make_async_copy(lists, lists_s, s_sem)
    to_scalars.start()
    ordered[ordered.shape[0] - 1] = jnp.zeros((TILE, LANES), jnp.float32)
    sums[:owners] = jnp.zeros((owners, TILE, LANES), jnp.float32)

    span = 32
    spans = block // span

    @pl.loop(0, n_chan * spans)
    def _(s):
        for when, some in ((spans, (1, 2, 3, 4)), (5 * spans, (5, 6)), (6 * spans, (7, 8))):

            @pl.when(s == when)
            def _(some=some):
                for n in some:
                    arrive(n)

        q = s // spans
        g = q // 3
        away = (1 + q) * (1 - g) * (2 - g) // 2 + (3 - q) * g * (2 - g) + (q - 2) * g * (g - 1) // 2
        r = lax.rem(chip * 2 + away + n_chan, n_chan)
        sub = lax.rem(s, spans)
        parity = lax.rem(r, 2)
        other = parity + core - 2 * parity * core
        row = (other * pairs + r // 2) * block + sub * span
        rows = pl.ds(pl.multiple_of(row, span), span)
        time = pl.multiple_of(r * block + sub * span, span)
        for lane in range(wide // LANES):
            lanes = slice(lane * LANES, (lane + 1) * LANES)
            past = series[pl.ds(time, pad + span), lanes]
            lagged = [past] + [pltpu.roll(past, TAP_SPACING * m, 0) for m in range(1, 4)]
            for b in range(bases):
                total = None
                for j in range(taps):
                    start = pad - TILE * (j // 4)
                    term = coef[b, j : j + 1, lanes] * lagged[j % 4][start : start + span]
                    total = term if total is None else total + term
                cols = slice(b * wide + lane * LANES, b * wide + (lane + 1) * LANES)
                design[rows, cols] = total.astype(design.dtype)

    mine = pairs * block

    def slab(i):
        return pl.ds(pl.multiple_of(i * SLAB, SLAB), SLAB)

    def way_cols(way, i):
        return pl.ds(pl.multiple_of(i * SLAB + way * half, half), half)

    def pair_copy(i):
        return pltpu.make_async_remote_copy(
            src_ref=dsend.at[:, slab(i)], dst_ref=drecv.at[:, slab(i)],
            send_sem=d_send.at[i], recv_sem=d_recv.at[i],
            device_id={"chan": device(0, 1)}, device_id_type=MESH,
        )

    def ring_copy(step, way, i):
        cols = way_cols(way, i)
        return pltpu.make_async_remote_copy(
            src_ref=rsend.at[step, :, cols], dst_ref=rrecv.at[step, :, cols],
            send_sem=r_send.at[step, way, i], recv_sem=r_recv.at[step, way, i],
            device_id={"chan": device((1, pairs - 1)[way], 0)}, device_id_type=MESH,
        )

    local_rows = LOCAL_TILES * TILE
    slab_groups = SLAB // SORT

    def sort_group(i, k, values):
        group = i * slab_groups + k
        spots = lax.broadcasted_iota(jnp.int32, (local_rows, LANES), 0)
        select = jnp.concatenate(
            [ones(spots == place[pl.ds(2 * group + h, 1), :]) for h in range(2)], axis=1
        )
        twice = jnp.concatenate([values, values], axis=0)
        rows = lax.dot_general(
            select, twice, (((1,), (1,)), ((), ())), preferred_element_type=jnp.float32
        )
        ordered[pl.ds(group * LOCAL_TILES, LOCAL_TILES)] = rows.reshape(LOCAL_TILES, TILE, LANES)
        added = lists_s.at[pl.ds(2 * owners + 2 * group, 1)]
        goes_on = lists_s.at[pl.ds(2 * owners + place.shape[0] + 2 * group, 1)]
        past = sums.at[pl.ds(group * owners, owners)]
        now = sums.at[pl.ds((group + 1) * owners, owners)]
        for o in range(owners):
            now[o] = past[o] * goes_on[0, o].astype(jnp.float32) + ordered[added[0, o]]

    def own_part(step, way, i):
        away = pairs - 1 - step if way == 0 else step + 1
        target = lax.rem(chip + away, pairs)
        return own[pl.ds(pl.multiple_of(target * block, block), block), way_cols(way, i)]

    def multiply(i):
        weight_copy(i).wait()
        for h in range(SLAB // 256):
            cols = pl.ds(pl.multiple_of(i * SLAB + h * 256, 256), 256)
            panel = wv[:, :, cols].reshape(bases * wide, 256)
            product = jnp.dot(design[...], panel, preferred_element_type=jnp.float32)
            dsend[:, cols] = product[mine:].astype(dsend.dtype)
            own[:, cols] = product[:mine]
        pair_copy(i).start()

    def pair_sum(i):
        pair_copy(i).wait_recv()
        own[:, slab(i)] = own[:, slab(i)] + drecv[:, slab(i)].astype(jnp.float32)

    def pass_on(step, i):
        for way in range(2):
            cols = way_cols(way, i)
            total = own_part(step, way, i)
            if step > 0:
                ring_copy(step - 1, way, i).wait_recv()
                total = total + rrecv[step - 1, :, cols].astype(jnp.float32)
            if step < pairs - 1:
                rsend[step, :, cols] = total.astype(rsend.dtype)
                ring_copy(step, way, i).start()
            else:
                sort_group(i, way, total.astype(jnp.bfloat16))

    to_scalars.wait()

    @pl.loop(0, steps + LAGS[-1])
    def _(it):
        @pl.when(it < steps)
        def _():
            multiply(it)

        for step in range(pairs):
            lag = LAGS[step]

            @pl.when(jnp.logical_and(it >= lag, it < steps + lag))
            def _(step=step, lag=lag):
                if step == 0:
                    pair_sum(it - lag)
                pass_on(step, it - lag)

    side = 4
    unit = ones(
        lax.broadcasted_iota(jnp.int32, (block, LANES), 0)
        == lax.broadcasted_iota(jnp.int32, (block, LANES), 1)
    )

    def fill(owner):
        unroll = 8
        opens = lists_s.at[pl.ds(owner, 1)]
        rest = lists_s.at[pl.ds(owners + owner, 1)]

        @pl.loop(0, cap // TILE // unroll)
        def _(s):
            for u in range(unroll):
                tile = s * unroll + u
                gathered[pl.ds(pl.multiple_of(tile * TILE, TILE), TILE), :] = (
                    ordered[opens[0, tile]] + sums[rest[0, tile]]
                )

        packed[owner] = lax.dot_general(
            unit, gathered[...].astype(jnp.bfloat16), (((1,), (1,)), ((), ())),
            preferred_element_type=jnp.float32,
        ).astype(packed.dtype)

    def peer_of(d):
        up_z, up_y = divmod(d, side)
        return lax.rem(here // side + up_z, owners // side) * side + lax.rem(here + up_y, side)

    def block_copy(d):
        return pltpu.make_async_remote_copy(
            src_ref=packed.at[peer_of(d)], dst_ref=out_ref.at[here],
            send_sem=x_send.at[d - 1], recv_sem=x_recv.at[d - 1],
            device_id={"vox": peer_of(d)}, device_id_type=MESH,
        )

    apart = {d: sum(min(k, side - k) for k in divmod(d, side)) for d in range(1, owners)}
    for d in sorted(apart, key=lambda d: -apart[d]):
        fill(peer_of(d))
        block_copy(d).start()
    fill(here)
    kept = pltpu.make_async_copy(packed.at[here], out_ref.at[here], x_local)
    kept.start()

    for n in range(len(parts)):
        feature_copy(n).wait_send()

    @pl.loop(0, steps)
    def _(i):
        pair_copy(i).wait_send()
        for step in range(pairs - 1):
            for way in range(2):
                ring_copy(step, way, i).wait_send()

    kept.wait()
    for d in range(1, owners):
        block_copy(d).wait()


def owned_block(features, hrf_filters, weights, voxel_parcel, parcel_owner, n_chan, owners):
    block, _ = features.shape
    bases, width, taps = hrf_filters.shape
    voxels = weights.shape[2]
    wide = up(width, LANES)
    steps = voxels // SLAB
    pairs = n_chan // 2
    cap = 2 * voxels // owners
    sizes = (n_chan, bases, taps, width, wide, block, steps, owners, cap)
    parcels = voxel_parcel.reshape(-1, LANES)
    sorted_tiles = voxels // SORT * LOCAL_TILES
    hbm = pl.BlockSpec(memory_space=pl.ANY)
    vmem = pl.BlockSpec(memory_space=pltpu.VMEM)
    dma = pltpu.SemaphoreType.DMA
    return pl.pallas_call(
        functools.partial(main_kernel, sizes),
        out_shape=pltpu.VMEM((owners, block, cap), jnp.bfloat16),
        in_specs=[hbm, hbm, hbm, vmem, vmem],
        out_specs=hbm,
        scratch_shapes=[
            pltpu.VMEM((bases, wide, voxels), jnp.bfloat16),
            pltpu.VMEM((n_chan, block, wide), jnp.bfloat16),
            pltpu.VMEM((32 + n_chan * block, wide), jnp.float32),
            pltpu.VMEM((bases, taps, width), jnp.float32),
            pltpu.VMEM((bases, taps, wide), jnp.float32),
            pltpu.VMEM((n_chan * block, bases * wide), jnp.bfloat16),
            pltpu.VMEM((pairs * block, voxels), jnp.float32),
            pltpu.VMEM((pairs * block, voxels), jnp.bfloat16),
            pltpu.VMEM((pairs * block, voxels), jnp.bfloat16),
            pltpu.VMEM((pairs - 1, block, voxels), jnp.bfloat16),
            pltpu.VMEM((pairs - 1, block, voxels), jnp.bfloat16),
            pltpu.VMEM(parcels.shape, jnp.int32),
            pltpu.VMEM((2 * owners + 2 * parcels.shape[0], LANES), jnp.int32),
            pltpu.SMEM((2 * owners + 2 * parcels.shape[0], LANES), jnp.int32),
            pltpu.VMEM((sorted_tiles + 1, TILE, LANES), jnp.float32),
            pltpu.VMEM(((voxels // SORT + 1) * owners, TILE, LANES), jnp.float32),
            pltpu.VMEM((cap, LANES), jnp.float32),
            pltpu.VMEM((owners, block, cap), jnp.bfloat16),
            dma((steps,)),
            dma,
            dma,
            dma((n_chan + 1,)),
            dma((n_chan + 1,)),
            dma((steps,)),
            dma((steps,)),
            dma((pairs - 1, 2, steps)),
            dma((pairs - 1, 2, steps)),
            dma,
            dma,
            dma((owners - 1,)),
            dma((owners - 1,)),
        ],
        compiler_params=pltpu.CompilerParams(
            collective_id=0, has_side_effects=True, vmem_limit_bytes=VMEM_LIMIT
        ),
        name="predict",
    )(features, hrf_filters.transpose(0, 2, 1), weights, parcels, parcel_owner)


def shards(features, hrf_filters, weights, voxel_parcel, parcel_owner):
    owners = lax.axis_size("vox")
    owned = owned_block(
        features, hrf_filters, weights, voxel_parcel, parcel_owner, lax.axis_size("chan"), owners
    )
    return owned.transpose(0, 2, 1)


def solution(mesh):
    return jax.shard_map(
        shards,
        mesh=mesh,
        in_specs=(P("chan", None), P(None, "chan", None), P(None, "chan", "vox"), P("vox"), P()),
        out_specs=P("vox", None, "chan"),
        check_vma=False,
    )
```
